512 devices in a mesh: row: 16 (over x, y), col: 32 (over z, core).
Axes of the slice: x: 4, y: 4, z: 16, core: 2. Of those that a mesh axis runs over, the one named last changes fastest.
Arguments:
- factors: float32 [1, 8192, 8192], P(None, 'row', 'col'), may hold values from -20 to 30, as said below
Outputs:
- refreshed: float32 [1, 8192, 8192], P(None, 'row', 'col')
The draws below stay inside these ranges and needn't reach their ends.
Inputs may be any that keep to these rules, and one draw needn't show every extreme that they name: `factors`: every factor is symmetric positive definite.
All inputs are finite; a program needn't handle non-finite values.
Results may differ from the reference program's by a relative error of at most 0.0003.
Values sent between devices are 32-bit elements; how exact they have to be, the bound alone decides.
A program may use at most 64 MiB of HBM per device.

```python
import jax
import jax.numpy as jnp
from jax import lax

N = 8192
P_SIZE = 512
STEPS = 2
FACTORS = 1
N_COL = 32


def draw_factors(key, part):
    base_key = jax.random.fold_in(key, 11)
    position = jnp.arange(N, dtype=jnp.float32)
    rising = 3.0 ** (0.5 * position / N)
    scale_low, scale_high = (0.25, 0.75)

    def one_factor(member):
        noise_key, level_key, scale_key, shared_key = jax.random.split(jax.random.fold_in(base_key, member), 4)
        jitter = jax.random.normal(noise_key, (N, N), jnp.float32)
        shared = 0.5 * jax.random.truncated_normal(shared_key, -2.0, 2.0, (N, 8), jnp.float32)
        symmetric = (jitter + jitter.T) * (0.5 / jnp.sqrt(2.0 * N))
        common_part = jnp.dot(shared, shared.T, precision=lax.Precision.HIGHEST)
        levels = jax.random.uniform(level_key, (N,), jnp.float32, 2.0, 4.0)
        scales = jnp.exp(jax.random.uniform(scale_key, (N,), jnp.float32, jnp.log(scale_low), jnp.log(scale_high))) * rising
        matrix_core = symmetric + common_part + jnp.diag(levels)
        return scales[:, None] * matrix_core * scales[None, :]
    return lax.map(one_factor, jnp.arange(FACTORS))


def setup_inputs(seed: int = 0) -> dict:
    arg_keys = jax.random.split(jax.random.key(seed), 2)
    factors = draw_factors(jax.random.fold_in(arg_keys[1], 71), 0)
    return dict(factors=factors)


damping_share = 0.03162277660168379

def reference(factors):
    col_block = N // N_COL
    panel_slab = P_SIZE // N_COL
    sequence = jnp.arange(N, dtype=jnp.int32).reshape(N // col_block, col_block // panel_slab, panel_slab)
    sequence = sequence.transpose(1, 0, 2).reshape(N)
    restore = jnp.zeros((N,), jnp.int32).at[sequence].set(jnp.arange(N, dtype=jnp.int32))
    results = []
    for member in range(FACTORS):
        matrix = factors[member]
        damping = damping_share * jnp.trace(matrix) / N
        matrix = matrix + damping * jnp.eye(N, dtype=matrix.dtype)
        matrix = matrix[sequence][:, sequence]
        for section_no in range(STEPS):
            begin_at = section_no * P_SIZE
            finish = begin_at + P_SIZE
            factor_kk = jnp.linalg.cholesky(matrix[begin_at:finish, begin_at:finish])
            inverse_kk = jax.scipy.linalg.solve_triangular(factor_kk, jnp.eye(P_SIZE, dtype=matrix.dtype), lower=True)
            panel_rows = jnp.dot(matrix[finish:, begin_at:finish], inverse_kk.T, precision=lax.Precision.HIGHEST)
            update = jnp.dot(panel_rows, panel_rows.T, precision=lax.Precision.HIGHEST)
            matrix = matrix.at[finish:, finish:].add(-update)
            matrix = matrix.at[begin_at:finish, begin_at:finish].set(factor_kk)
            matrix = matrix.at[finish:, begin_at:finish].set(panel_rows)
            matrix = matrix.at[begin_at:finish, finish:].set(0.0)
        results.append(matrix[restore][:, restore])
    return jnp.stack(results)
```

```python
import jax, jax.numpy as jnp
from jax import lax
from jax.experimental import pallas as pl
from jax.experimental.pallas import tpu as pltpu
from jax.sharding import PartitionSpec as P

F32, BF16 = jnp.float32, jnp.bfloat16
damping_share = 0.03162277660168379

def split3(x):
    h = x.astype(BF16)
    r = x - h.astype(F32)
    m = r.astype(BF16)
    l = (r - m.astype(F32)).astype(BF16)
    return h, m, l

def split2(x):
    h = x.astype(BF16)
    return h, (x - h.astype(F32)).astype(BF16)

def tn(a, b):
    return lax.dot_general(a, b, (((0,), (0,)), ((), ())), preferred_element_type=F32)

def nn(a, b):
    return lax.dot_general(a, b, (((1,), (0,)), ((), ())), preferred_element_type=F32)

def block_inverse(M, b=16):
    n = 128
    H = b // 8
    sub = lax.broadcasted_iota(jnp.int32, (8, n), 0)
    lane = lax.broadcasted_iota(jnp.int32, (8, n), 1)
    M = [M[8 * i:8 * i + 8, :] for i in range(n // 8)]
    for s in range(n // b):
        r0 = s * b
        q0 = r0 // 8
        S = [[None] * b for _ in range(H)]
        for k in range(b):
            for h in range(k // 8, H):
                S[h][k] = jnp.broadcast_to(M[q0 + h][:, r0 + k:r0 + k + 1], (8, n))
        inblk = (lane >= r0) & (lane < r0 + b)
        N = [jnp.where(inblk, jnp.where(lane - r0 == sub + 8 * h, 1.0, 0.0).astype(F32), M[q0 + h]) for h in range(H)]
        scale = [None] * H
        for j in range(b):
            hj, sj = j // 8, j % 8
            piv = jnp.broadcast_to(S[hj][j][sj:sj + 1, :], (8, n))
            rs = lax.rsqrt(piv)
            rinv = rs * rs
            scale[hj] = rs if sj == 0 else jnp.where(sub == sj, rs, scale[hj])
            if j == b - 1:
                break
            for k in range(j + 1, b):
                hk, sk = k // 8, k % 8
                t = jnp.broadcast_to(S[hk][j][sk:sk + 1, :], (8, n)) * rinv
                for h in range(hk, H):
                    S[h][k] = S[h][k] - S[h][j] * t
            prow = jnp.broadcast_to(N[hj][sj:sj + 1, :], (8, n)) * rinv
            for h in range(hj, H):
                if h == hj:
                    if sj == 7:
                        continue
                    N[h] = jnp.where(sub > sj, N[h] - S[h][j] * prow, N[h])
                else:
                    N[h] = N[h] - S[h][j] * prow
        Y = jnp.concatenate([N[h] * scale[h] for h in range(H)], axis=0)
        lb = lax.broadcasted_iota(jnp.int32, (b, n), 1)
        for h in range(H):
            M[q0 + h] = Y[8 * h:8 * h + 8, :] if s == n // b - 1 else jnp.where(lane < r0 + b, Y[8 * h:8 * h + 8, :], 0.0)
        if s < n // b - 1:
            h_, m_, l_ = split3(Y)
            R = tn(jnp.concatenate([h_, h_, m_, h_, l_, m_], 0), jnp.concatenate([h_, m_, h_, l_, h_, m_], 0))
            for q in range(q0 + H, n // 8):
                M[q] = jnp.where(inblk, 0.0, M[q]) - R[8 * q:8 * q + 8, :]
    return jnp.concatenate(M, axis=0)

NBLK = 8
NB = 128
KK = 1024
LB = 768

def cat3l(h, l):
    return jnp.concatenate([h, l, h], axis=1)

def cat3r(h, l):
    return jnp.concatenate([h, h, l], axis=0)

def compute_kernel(damp_ref, akk_ref, bc_ref, br_ref, a_ref, out_ref, g, yb, w_ref, tl_ref, rh_ref, u_ref):
    i_row = lax.axis_index("row")
    j_col = lax.axis_index("col")
    damp = damp_ref[0:1, :]
    damp2 = jnp.concatenate([damp, damp], axis=1)
    damp4 = jnp.concatenate([damp2, damp2], axis=1)
    g[:, 0:KK] = akk_ref[...]
    g[:, KK:KK + 256] = bc_ref[...]
    posr = lax.broadcasted_iota(jnp.int32, (KK, 512), 0)
    ln = lax.broadcasted_iota(jnp.int32, (KK, 512), 1)
    lm = ln % 256
    posl = jnp.where(lm < 32, (lm // 16) * 512 + (2 * i_row + ln // 256) * 16 + lm % 16, -1)
    g[:, KK + 256:] = br_ref[...] + jnp.where(posr == posl, damp4, 0.0)

    eye = (lax.broadcasted_iota(jnp.int32, (NB, NB), 0) == lax.broadcasted_iota(jnp.int32, (NB, NB), 1))

    def body(b, carry):
        o = pl.multiple_of(b * NB, NB)
        D = g[pl.ds(o, NB), pl.ds(o, NB)] + jnp.where(eye, damp, 0.0)
        w_ref[...] = block_inverse(D)
        for k in range(NBLK):
            @pl.when(b == k)
            def _():
                lo = (k + 1) * NB
                W = w_ref[...]
                wl = cat3l(*split2(W))
                r0 = k * NB
                G = g[r0:r0 + NB, lo:]
                Y = nn(wl, cat3r(*split2(G)))
                g[r0:r0 + NB, lo:] = Y
                if k < NBLK - 1:
                    Mr = KK - lo
                    h, l = split2(Y)
                    lhs = cat3r(h[:, :Mr], l[:, :Mr])
                    lhs = jnp.concatenate([h[:, :Mr], l[:, :Mr], h[:, :Mr]], 0)
                    rhs = cat3r(h, l)
                    tl_ref[:, 0:Mr] = lhs
                    rh_ref[:, 0:KK - lo + LB] = rhs
                    ntile = (KK - lo + LB) // 128
                    def upd(c, _):
                        oo = pl.multiple_of(c * 128, 128)
                        R = tn(tl_ref[:, 0:Mr], rh_ref[:, pl.ds(oo, 128)])
                        gl = pl.ds(pl.multiple_of(oo + lo, 128), 128)
                        g[lo:, gl] = g[lo:, gl] - R
                        return 0
                    lax.fori_loop(0, ntile, upd, 0)
        return carry
    lax.fori_loop(0, NBLK, body, 0)

    U = None
    for t in range(4):
        sl = slice(t * 256, t * 256 + 256)
        rh, rl = split2(g[sl, KK + 256:])
        ch, cl = split2(g[sl, KK:KK + 256])
        P = tn(jnp.concatenate([rh, rl, rh], 0), jnp.concatenate([ch, ch, cl], 0))
        U = P if U is None else U + P
    p0 = g[pl.ds(pl.multiple_of(j_col * 16, 16), 16), KK + 256:]
    p1 = g[pl.ds(pl.multiple_of(512 + j_col * 16, 16), 16), KK + 256:]
    pt = jnp.concatenate([p0, p1, jnp.zeros((96, 512), F32)], 0).T
    r = lax.broadcasted_iota(jnp.int32, (512, 256), 0)
    c = lax.broadcasted_iota(jnp.int32, (512, 256), 1)
    rm = r % 256
    posrow = jnp.where(rm < 32, (rm // 16) * 512 + (2 * i_row + r // 256) * 16 + rm % 16, KK)
    poscol = (c // 16) * 512 + j_col * 16 + c % 16
    A = a_ref[...]
    A = A + jnp.where(r + 512 * i_row == c + 256 * j_col, damp2, 0.0)
    ptw = jnp.concatenate([pt, jnp.zeros((512, 128), F32)], 1)
    out = jnp.where(c >= 32, jnp.where(rm >= 32, A - U, 0.0), jnp.where(posrow >= poscol, ptw, 0.0))
    out_ref[...] = out

def compute(damp, akk, bc, br, a):
    vm = pl.BlockSpec(memory_space=pltpu.VMEM)
    return pl.pallas_call(
        compute_kernel,
        out_shape=jax.ShapeDtypeStruct((512, 256), F32),
        in_specs=[vm] * 5,
        out_specs=vm,
        scratch_shapes=[pltpu.VMEM((KK, KK + LB), F32), pltpu.VMEM((8, 128), F32), pltpu.VMEM((NB, NB), F32),
                        pltpu.VMEM((384, KK - NB), BF16), pltpu.VMEM((384, KK - NB + LB), BF16), pltpu.VMEM((8, 128), F32)],
        compiler_params=pltpu.CompilerParams(vmem_limit_bytes=60 * 1024 * 1024),
        name="eliminate",
    )(damp, akk, bc, br, a)


MESH = pl.DeviceIdType.MESH


def comm_kernel(a_ref, akk, bc, br, damp_ref, zb, tr, bar_unused, zs, zr, zd, xs, xr, ks, kr, kd, us, ur, ds, dr, dd):
    i = lax.axis_index("row")
    j = lax.axis_index("col")
    z = j // 2
    c = lax.rem(j, 2)
    me_partner = (i, 2 * z + 1 - c)

    def zpeer(d):
        return (i, 2 * lax.rem(z + d, 16) + c)

    def xpeer(d):
        return (lax.rem(i + d, 16), j)

    barrier = pltpu.get_barrier_semaphore()

    def greet(d, carry):
        pl.semaphore_signal(barrier, inc=1, device_id=zpeer(d), device_id_type=MESH)
        pl.semaphore_signal(barrier, inc=1, device_id=xpeer(d), device_id_type=MESH)
        return carry

    lax.fori_loop(1, 16, greet, 0)
    pl.semaphore_signal(barrier, inc=1, device_id=me_partner, device_id_type=MESH)

    T = a_ref[:, 0:128].T
    br[0, z, c] = T[0:16, :]
    br[1, z, c] = T[16:32, :]
    lane = lax.broadcasted_iota(jnp.int32, (16, 128), 1)
    x0, y0 = T[0:16, 0:128], T[0:16, 256:384]
    x1, y1 = T[16:32, 0:128], T[16:32, 256:384]
    piece = jnp.where(
        lane < 32,
        x0,
        jnp.where(lane < 64, pltpu.roll(y0, 32, 1), jnp.where(lane < 96, pltpu.roll(x1, 64, 1), pltpu.roll(y1, 96, 1))),
    )
    zb[z, c, 0:16, :] = piece
    r = lax.broadcasted_iota(jnp.int32, (512, 256), 0)
    q = lax.broadcasted_iota(jnp.int32, (512, 256), 1)
    on = r + 512 * i == q + 256 * j
    t = jnp.sum(jnp.where(on, a_ref[...], 0.0), axis=0, keepdims=True)
    t = jnp.sum(t, axis=1, keepdims=True)
    zb[z, c, 16:24, :] = jnp.broadcast_to(t, (8, 128))
    for p in range(2):
        for h in range(2):
            bc[p, i, h] = a_ref[256 * h + 16 * p : 256 * h + 16 * p + 16, :]

    pl.semaphore_wait(barrier, 31)

    def z_send(d):
        return pltpu.make_async_remote_copy(
            src_ref=zb.at[z, c], dst_ref=zb.at[z, c], send_sem=zs.at[d], recv_sem=zr.at[d],
            device_id=zpeer(d), device_id_type=MESH)

    def z_recv(d):
        s = lax.rem(z + 16 - d, 16)
        return pltpu.make_async_remote_copy(
            src_ref=zb.at[s, c], dst_ref=zb.at[s, c], send_sem=zs.at[d], recv_sem=zr.at[d],
            device_id=zpeer(d), device_id_type=MESH)

    def x_send(d):
        return pltpu.make_async_remote_copy(
            src_ref=bc.at[:, i], dst_ref=bc.at[:, i], send_sem=xs.at[d], recv_sem=xr.at[d],
            device_id=xpeer(d), device_id_type=MESH)

    def x_recv(d):
        s = lax.rem(i + 16 - d, 16)
        return pltpu.make_async_remote_copy(
            src_ref=bc.at[:, s], dst_ref=bc.at[:, s], send_sem=xs.at[d], recv_sem=xr.at[d],
            device_id=xpeer(d), device_id_type=MESH)

    up_to = (i, 2 * lax.rem(z + 1, 16) + c)
    down_to = (i, 2 * lax.rem(z + 15, 16) + c)

    def ring(s, up):
        k = lax.rem(z + 16 - s, 16) if up else lax.rem(z + s, 16)
        o = 0 if up else 8
        return pltpu.make_async_remote_copy(
            src_ref=br.at[:, k, c], dst_ref=br.at[:, k, c], send_sem=us.at[s + o], recv_sem=ur.at[s + o],
            device_id=up_to if up else down_to, device_id_type=MESH)

    def ring_in(s, up):
        k = lax.rem(z + 15 - s, 16) if up else lax.rem(z + 1 + s, 16)
        o = 0 if up else 8
        return pltpu.make_async_remote_copy(
            src_ref=br.at[:, k, c], dst_ref=br.at[:, k, c], send_sem=us.at[s + o], recv_sem=ur.at[s + o],
            device_id=up_to if up else down_to, device_id_type=MESH)

    def pair(k):
        return pltpu.make_async_remote_copy(
            src_ref=br.at[:, k, c], dst_ref=br.at[:, k, c], send_sem=ds.at[k], recv_sem=dr.at[k],
            device_id=me_partner, device_id_type=MESH)

    def pair_in(k):
        return pltpu.make_async_remote_copy(
            src_ref=br.at[:, k, 1 - c], dst_ref=br.at[:, k, 1 - c], send_sem=ds.at[k], recv_sem=dr.at[k],
            device_id=me_partner, device_id_type=MESH)

    def go(f):
        def step(d, carry):
            f(d)
            return carry
        return step

    lax.fori_loop(1, 16, go(lambda d: z_send(d).start()), 0)
    ring(0, True).start()
    ring(0, False).start()
    pair(z).start()
    lax.fori_loop(1, 16, go(lambda d: x_send(d).start()), 0)

    def ring_step(s, last=False):
        ring_in(s - 1, True).wait_recv()
        ring(s, True).start()
        pair(lax.rem(z + 16 - s, 16)).start()
        ring_in(s - 1, False).wait_recv()
        if not last:
            ring(s, False).start()
        pair(lax.rem(z + s, 16)).start()

    for s in (1, 2):
        ring_step(s)

    lax.fori_loop(1, 16, go(lambda d: z_recv(d).wait_recv()), 0)
    zpair = pltpu.make_async_remote_copy(
        src_ref=zb.at[:, c], dst_ref=zb.at[:, c], send_sem=zd.at[0], recv_sem=zd.at[1],
        device_id=me_partner, device_id_type=MESH)
    zpair.start()
    pltpu.make_async_remote_copy(
        src_ref=zb.at[:, 1 - c], dst_ref=zb.at[:, 1 - c], send_sem=zd.at[0], recv_sem=zd.at[1],
        device_id=me_partner, device_id_type=MESH).wait_recv()
    G = zb[:, :, 0:16, :].reshape(512, 128).T
    rowsum = jnp.sum(zb[:, :, 16:24, :].reshape(32, 8, 128), axis=0)
    tr[i] = rowsum
    akk[0, i, c, :, 0:512] = jnp.where(c == 0, G[0:16, :], G[32:48, :])
    akk[0, i, c, :, 512:1024] = jnp.where(c == 0, G[64:80, :], G[96:112, :])
    akk[1, i, c, :, 512:1024] = jnp.where(c == 0, G[80:96, :], G[112:128, :])

    def k_copy(d, s, n):
        src = (akk.at[0, s, c], akk.at[1, s, c, :, pl.ds(512, 512)], tr.at[s])[n]
        return pltpu.make_async_remote_copy(
            src_ref=src, dst_ref=src, send_sem=ks.at[n, d], recv_sem=kr.at[n, d],
            device_id=xpeer(d), device_id_type=MESH)

    for n in range(3):
        lax.fori_loop(1, 16, go(lambda d: k_copy(d, i, n).start()), 0)
    for s in range(3, 7):
        ring_step(s)
    ring_step(7, last=True)

    for n in range(3):
        lax.fori_loop(1, 16, go(lambda d: k_copy(d, lax.rem(i + 16 - d, 16), n).wait_recv()), 0)

    def kpair(n, h):
        src = (akk.at[0, :, h], akk.at[1, :, h, :, pl.ds(512, 512)])[n]
        return pltpu.make_async_remote_copy(
            src_ref=src, dst_ref=src, send_sem=kd.at[n], recv_sem=kd.at[2 + n],
            device_id=me_partner, device_id_type=MESH)

    kpair(0, c).start()
    kpair(1, c).start()
    damp_ref[...] = jnp.sum(tr[...], axis=0) * (damping_share / 8192.0)

    ring_in(7, True).wait_recv()
    pair(lax.rem(z + 8, 16)).start()
    lax.fori_loop(1, 16, go(lambda d: x_recv(d).wait_recv()), 0)
    lax.fori_loop(0, 16, go(lambda k: pair_in(k).wait_recv()), 0)
    kpair(0, 1 - c).wait_recv()
    kpair(1, 1 - c).wait_recv()

    lax.fori_loop(1, 16, go(lambda d: z_send(d).wait_send()), 0)
    lax.fori_loop(1, 16, go(lambda d: x_send(d).wait_send()), 0)
    for n in range(3):
        lax.fori_loop(1, 16, go(lambda d: k_copy(d, i, n).wait_send()), 0)
    for s in range(8):
        ring(s, True).wait_send()
        if s < 7:
            ring(s, False).wait_send()
    lax.fori_loop(0, 16, go(lambda k: pair(k).wait_send()), 0)
    zpair.wait_send()
    kpair(0, c).wait_send()
    kpair(1, c).wait_send()


def gather(a):
    vm = pl.BlockSpec(memory_space=pltpu.VMEM)
    dma = pltpu.SemaphoreType.DMA
    return pl.pallas_call(
        comm_kernel,
        out_shape=[
            jax.ShapeDtypeStruct((2, 16, 2, 16, 1024), F32),
            jax.ShapeDtypeStruct((2, 16, 2, 16, 256), F32),
            jax.ShapeDtypeStruct((2, 16, 2, 16, 512), F32),
            jax.ShapeDtypeStruct((8, 128), F32),
        ],
        in_specs=[vm],
        out_specs=[vm] * 4,
        scratch_shapes=[
            pltpu.VMEM((16, 2, 24, 128), F32), pltpu.VMEM((16, 8, 128), F32), pltpu.VMEM((8, 128), F32),
            dma((16,)), dma((16,)), dma((2,)), dma((16,)), dma((16,)), dma((3, 16)), dma((3, 16)), dma((4,)),
            dma((16,)), dma((16,)), dma((16,)), dma((16,)), dma((1,)),
        ],
        compiler_params=pltpu.CompilerParams(collective_id=0, has_side_effects=True, vmem_limit_bytes=32 * 1024 * 1024),
        name="gather",
    )(a)


def on_device(factors):
    a = factors[0]
    akk, bc, br, damp = gather(a)
    out = compute(damp, akk.reshape(1024, 1024), bc.reshape(1024, 256), br.reshape(1024, 512), a)
    return out[None]


def solution(mesh):
    placed = P(None, "row", "col")
    return jax.shard_map(on_device, mesh=mesh, in_specs=(placed,), out_specs=placed, check_vma=False)
```

```python
import jax
import jax.numpy as jnp
from jax import lax
from jax.experimental import pallas as pl
from jax.experimental.pallas import tpu as pltpu
from jax.sharding import PartitionSpec as P

F32, BF16 = jnp.float32, jnp.bfloat16
MESH = pl.DeviceIdType.MESH
damping_share = 0.03162277660168379
NB = 128
MINI = 32
PS = 512
RW = PS + 256 + 512


def split3(x):
    h = x.astype(BF16)
    r = x - h.astype(F32)
    m = r.astype(BF16)
    return h, m, (r - m.astype(F32)).astype(BF16)


def split2(x):
    h = x.astype(BF16)
    return h, (x - h.astype(F32)).astype(BF16)


def tn(a, b):
    return lax.dot_general(a, b, (((0,), (0,)), ((), ())), preferred_element_type=F32)


def nn(a, b):
    return lax.dot_general(a, b, (((1,), (0,)), ((), ())), preferred_element_type=F32)


def left3(h, l):
    return jnp.concatenate([h, l, h], axis=1)


def right3(h, l):
    return jnp.concatenate([h, h, l], axis=0)


def block_inverse(M, b=MINI):
    n = 128
    H = b // 8
    sub = lax.broadcasted_iota(jnp.int32, (8, n), 0)
    lane = lax.broadcasted_iota(jnp.int32, (8, n), 1)
    M = [M[8 * i:8 * i + 8, :] for i in range(n // 8)]
    for s in range(n // b):
        r0 = s * b
        q0 = r0 // 8
        S = [[None] * b for _ in range(H)]
        for k in range(b):
            for h in range(k // 8, H):
                S[h][k] = jnp.broadcast_to(M[q0 + h][:, r0 + k:r0 + k + 1], (8, n))
        inblk = (lane >= r0) & (lane < r0 + b)
        N = [jnp.where(inblk, jnp.where(lane - r0 == sub + 8 * h, 1.0, 0.0).astype(F32), M[q0 + h]) for h in range(H)]
        scale = [None] * H
        for j in range(b):
            hj, sj = j // 8, j % 8
            piv = jnp.broadcast_to(S[hj][j][sj:sj + 1, :], (8, n))
            rs = lax.rsqrt(piv)
            rinv = rs * rs
            scale[hj] = rs if sj == 0 else jnp.where(sub == sj, rs, scale[hj])
            if j == b - 1:
                break
            for k in range(j + 1, b):
                hk, sk = k // 8, k % 8
                t = jnp.broadcast_to(S[hk][j][sk:sk + 1, :], (8, n)) * rinv
                for h in range(hk, H):
                    S[h][k] = S[h][k] - S[h][j] * t
            prow = jnp.broadcast_to(N[hj][sj:sj + 1, :], (8, n)) * rinv
            for h in range(hj, H):
                if h == hj:
                    if sj == 7:
                        continue
                    N[h] = jnp.where(sub > sj, N[h] - S[h][j] * prow, N[h])
                else:
                    N[h] = N[h] - S[h][j] * prow
        Y = jnp.concatenate([N[h] * scale[h] for h in range(H)], axis=0)
        lb = lax.broadcasted_iota(jnp.int32, (b, n), 1)
        for h in range(H):
            M[q0 + h] = Y[8 * h:8 * h + 8, :] if s == n // b - 1 else jnp.where(lane < r0 + b, Y[8 * h:8 * h + 8, :], 0.0)
        if s < n // b - 1:
            h_, m_, l_ = split3(Y)
            R = tn(jnp.concatenate([h_, h_, m_, h_, l_, m_], 0), jnp.concatenate([h_, m_, h_, l_, h_, m_], 0))
            for q in range(q0 + H, n // 8):
                M[q] = jnp.where(inblk, 0.0, M[q]) - R[8 * q:8 * q + 8, :]
    return jnp.concatenate(M, axis=0)

def kernel(a_ref, out_ref, akk, bc, br, zb, tz, tx, dn, wst, lh, ll, kh, kl, g0, g1, ph, pm, qh, ql, y0, y1, w_ref,
           zs, zr, zd, ts, tr, xs, xr, ks, kr, kd, hs, hr, us, ur, ds, dr):
    i = lax.axis_index("row")
    j = lax.axis_index("col")
    z = j // 2
    c = lax.rem(j, 2)
    partner = (i, 2 * z + 1 - c)

    def zpeer(d):
        return (i, 2 * lax.rem(z + d, 16) + c)

    def xpeer(d):
        return (lax.rem(i + d, 16), j)

    def copy(src, dst, ssem, rsem, dev):
        return pltpu.make_async_remote_copy(
            src_ref=src, dst_ref=dst, send_sem=ssem, recv_sem=rsem, device_id=dev, device_id_type=MESH)

    def each(lo, hi, f):
        def step(d, carry):
            f(d)
            return carry
        lax.fori_loop(lo, hi, step, 0)

    barrier = pltpu.get_barrier_semaphore()

    def greet(d):
        pl.semaphore_signal(barrier, inc=1, device_id=zpeer(d), device_id_type=MESH)
        pl.semaphore_signal(barrier, inc=1, device_id=xpeer(d), device_id_type=MESH)

    each(1, 16, greet)
    pl.semaphore_signal(barrier, inc=1, device_id=partner, device_id_type=MESH)

    T = a_ref[:, 0:128].T
    br[0, z, c] = T[0:16, :]
    br[1, z, c] = T[16:32, :]
    lane = lax.broadcasted_iota(jnp.int32, (16, 128), 1)
    p0, p1 = T[0:16, 0:128], T[0:16, 256:384]
    p2, p3 = T[16:32, 0:128], T[16:32, 256:384]
    zb[z, c] = jnp.where(
        lane < 32, p0,
        jnp.where(lane < 64, pltpu.roll(p1, 32, 1), jnp.where(lane < 96, pltpu.roll(p2, 64, 1), pltpu.roll(p3, 96, 1))))
    r = lax.broadcasted_iota(jnp.int32, (512, 256), 0)
    q = lax.broadcasted_iota(jnp.int32, (512, 256), 1)
    on_diagonal = r + 512 * i == q + 256 * j
    t = jnp.sum(jnp.where(on_diagonal, a_ref[...], 0.0), axis=0, keepdims=True)
    tz[z, c] = jnp.broadcast_to(jnp.sum(t, axis=1, keepdims=True), (1, 128))
    for p in range(2):
        for h in range(2):
            bc[p, i, h] = a_ref[256 * h + 16 * p : 256 * h + 16 * p + 16, :]

    pl.semaphore_wait(barrier, 31)

    def behind(v, d):
        return lax.rem(v + 16 - d, 16)

    def z_copy(d, s):
        return copy(zb.at[s, c], zb.at[s, c], zs.at[d], zr.at[d], zpeer(d))

    def t_copy(d, s):
        return copy(tz.at[s, c], tz.at[s, c], ts.at[d], tr.at[d], zpeer(d))

    def x_copy(d, s):
        return copy(bc.at[:, s], bc.at[:, s], xs.at[d], xr.at[d], xpeer(d))

    def h_copy(d, s):
        return copy(tx.at[s], tx.at[s], hs.at[d], hr.at[d], xpeer(d))

    def strip(n, s, h):
        return (akk.at[0, s, h, :, pl.ds(0, 512)], akk.at[0, s, h, :, pl.ds(512, 512)],
                akk.at[1, s, h, :, pl.ds(512, 512)])[n]

    def k_copy(n, d, s):
        return copy(strip(n, s, c), strip(n, s, c), ks.at[n, d], kr.at[n, d], xpeer(d))

    def k_pair(n, h):
        v = (akk.at[0, :, h, :, pl.ds(0, 512)], akk.at[0, :, h, :, pl.ds(512, 512)],
             akk.at[1, :, h, :, pl.ds(512, 512)])[n]
        return copy(v, v, kd.at[n], kd.at[3 + n], partner)

    def z_pair(h):
        return copy(zb.at[:, h], zb.at[:, h], zd.at[0], zd.at[1], partner)

    def t_pair(h):
        return copy(tz.at[:, h], tz.at[:, h], zd.at[2], zd.at[3], partner)

    up_to = (i, 2 * lax.rem(z + 1, 16) + c)
    down_to = (i, 2 * lax.rem(z + 15, 16) + c)

    def ring(s, up, arriving=False):
        e = s + 1 if arriving else s
        k = behind(z, e) if up else lax.rem(z + e, 16)
        o = 0 if up else 8
        return copy(br.at[:, k, c], br.at[:, k, c], us.at[s + o], ur.at[s + o], up_to if up else down_to)

    def pair(k, h):
        return copy(br.at[:, k, h], br.at[:, k, h], ds.at[k], dr.at[k], partner)

    def ring_step(s):
        ring(s - 1, True, True).wait_recv()
        ring(s, True).start()
        pair(behind(z, s), c).start()
        ring(s - 1, False, True).wait_recv()
        if s < 7:
            ring(s, False).start()
        pair(lax.rem(z + s, 16), c).start()

    each(1, 16, lambda d: z_copy(d, z).start())
    each(1, 16, lambda d: t_copy(d, z).start())
    ring(0, True).start()
    ring(0, False).start()
    pair(z, c).start()

    each(1, 16, lambda d: t_copy(d, behind(z, d)).wait_recv())
    t_pair(c).start()
    each(1, 16, lambda d: z_copy(d, behind(z, d)).wait_recv())
    z_pair(c).start()
    t_pair(1 - c).wait_recv()
    tx[i] = jnp.sum(tz[...].reshape(32, 1, 128), axis=0)
    each(1, 16, lambda d: h_copy(d, i).start())
    z_pair(1 - c).wait_recv()
    S = zb[...].reshape(512, 128).T
    akk[0, i, c, :, 0:512] = jnp.where(c == 0, S[0:16, :], S[32:48, :])
    akk[0, i, c, :, 512:1024] = jnp.where(c == 0, S[64:80, :], S[96:112, :])
    akk[1, i, c, :, 512:1024] = jnp.where(c == 0, S[80:96, :], S[112:128, :])
    each(1, 16, lambda d: k_copy(0, d, i).start())
    each(1, 16, lambda d: k_copy(1, d, i).start())
    each(1, 16, lambda d: x_copy(d, i).start())
    each(1, 16, lambda d: k_copy(2, d, i).start())
    ring_step(1)
    ring_step(2)
    each(1, 16, lambda d: h_copy(d, behind(i, d)).wait_recv())
    damp = jnp.sum(tx[...], axis=0) * (damping_share / 8192.0)
    each(1, 16, lambda d: k_copy(0, d, behind(i, d)).wait_recv())
    k_pair(0, c).start()
    ring_step(3)
    k_pair(0, 1 - c).wait_recv()

    damp2 = jnp.concatenate([damp, damp], axis=1)
    damp4 = jnp.concatenate([damp2, damp2], axis=1)
    eye = lax.broadcasted_iota(jnp.int32, (NB, NB), 0) == lax.broadcasted_iota(jnp.int32, (NB, NB), 1)
    deye = jnp.where(eye, damp, 0.0)
    ln = lax.broadcasted_iota(jnp.int32, (PS, 512), 1)
    posl = jnp.where(ln % 256 < 32, (ln % 256 // 16) * 512 + (2 * i + ln // 256) * 16 + ln % 16, -1)
    posr = lax.broadcasted_iota(jnp.int32, (PS, 512), 0)

    g0[...] = akk[0, :, :, :, 0:512].reshape(512, 512)
    dn[...] = g0[0:NB, 0:NB]

    def middle():
        ring(7, True, True).wait_recv()
        pair(lax.rem(z + 8, 16), c).start()
        each(1, 16, lambda d: k_copy(1, d, behind(i, d)).wait_recv())
        k_pair(1, c).start()
        each(1, 16, lambda d: x_copy(d, behind(i, d)).wait_recv())
        each(1, 16, lambda d: k_copy(2, d, behind(i, d)).wait_recv())
        k_pair(2, c).start()
        each(0, 16, lambda k: pair(k, 1 - c).wait_recv())
        k_pair(1, 1 - c).wait_recv()
        k_pair(2, 1 - c).wait_recv()
        for b in range(4):
            o = b * NB
            rows = slice(o, o + NB)
            acc = jnp.concatenate([
                akk[0, 4 * b : 4 * b + 4, :, :, 512:1024].reshape(NB, 512),
                bc[0, 4 * b : 4 * b + 4].reshape(NB, 256),
                br[0, 4 * b : 4 * b + 4].reshape(NB, 512) + jnp.where(posr[rows] == posl[rows], damp4, 0.0)], axis=1)
            if b:
                acc = acc - nn(
                    jnp.concatenate([lh[rows, 0:o], ll[rows, 0:o], lh[rows, 0:o]], axis=1),
                    jnp.concatenate([ph[0:o, :], ph[0:o, :], pm[0:o, :]], axis=0))
            Y = nn(wst[b], right3(*split2(acc)))
            y0[rows, :] = Y[:, PS + 256 :]
            ph[rows, :], pm[rows, :] = split2(Y)
            th, tl = split2(Y[:, 0:PS].T)
            kh[:, o : o + NB] = th
            kl[:, o : o + NB] = tl
        left = jnp.concatenate([kh[...], kl[...], kh[...]], axis=1)
        for o in range(0, RW, 256):
            R = nn(left, jnp.concatenate([ph[:, o : o + 256], ph[:, o : o + 256], pm[:, o : o + 256]], axis=0))
            if o < PS:
                src = akk[1, :, :, :, 512 + o : 768 + o].reshape(512, 256)
            elif o == PS:
                src = bc[1].reshape(512, 256)
            else:
                v = o - PS - 256
                src = br[1, :, :, :, v : v + 256].reshape(512, 256) + jnp.where(
                    posr[:, v : v + 256] + 512 == posl[:, v : v + 256], damp2, 0.0)
            g1[:, o : o + 256] = src - R
        dn[...] = g1[0:NB, 0:NB]

    def body(b, carry):
        w_ref[...] = block_inverse(dn[...] + deye)
        for k in range(8):

            @pl.when(b == k)
            def _():
                wl = left3(*split2(w_ref[...]))
                kk = k % 4
                lo = (kk + 1) * NB
                rows = slice(kk * NB, lo)
                if k < 4:
                    wst[k] = wl
                    ring_step(4 + k)
                    if k == 3:
                        middle()
                        return
                    g, hi = g0, PS
                else:
                    g, hi = g1, RW
                Y = nn(wl, right3(*split2(g[rows, lo:hi])))
                h, l = split2(Y)
                if k >= 4:
                    y1[rows, :] = Y[:, PS + 256 - lo :]
                    qh[rows, :] = h[:, PS - lo :]
                    ql[rows, :] = l[:, PS - lo :]
                if kk < 3:
                    th, tl = split2(Y[:, 0 : PS - lo].T)
                    if k < 4:
                        lh[lo:PS, rows] = th
                        ll[lo:PS, rows] = tl
                    left = left3(th, tl)
                    right = right3(h, l)
                    for o in range(0, hi - lo, 256):
                        e = min(o + 256, hi - lo)
                        g[lo:PS, lo + o : lo + e] = g[lo:PS, lo + o : lo + e] - nn(left, right[:, o:e])
                    dn[...] = g[lo : lo + NB, lo : lo + NB]
        return carry

    lax.fori_loop(0, 8, body, 0)

    U = None
    for yh, yl, base in ((ph, pm, PS), (qh, ql, 0)):
        for o in (0, 256):
            s = slice(o, o + 256)
            rh, rl = yh[s, base + 256 :], yl[s, base + 256 :]
            ch, cl = yh[s, base : base + 256], yl[s, base : base + 256]
            X = tn(jnp.concatenate([rh, rl, rh], 0), jnp.concatenate([ch, ch, cl], 0))
            U = X if U is None else U + X
    at = pl.ds(pl.multiple_of(j * 16, 16), 16)
    cols = jnp.concatenate([y0[at, :], y1[at, :], jnp.zeros((96, 512), F32)], 0).T
    rm = r % 256
    posrow = jnp.where(rm < 32, (rm // 16) * 512 + (2 * i + r // 256) * 16 + rm % 16, 1024)
    poscol = (q // 16) * 512 + j * 16 + q % 16
    A = a_ref[...] + jnp.where(on_diagonal, damp2, 0.0)
    cols = jnp.concatenate([cols, jnp.zeros((512, 128), F32)], 1)
    out_ref[...] = jnp.where(
        q >= 32, jnp.where(rm >= 32, A - U, 0.0), jnp.where(posrow >= poscol, cols, 0.0))

    each(1, 16, lambda d: z_copy(d, z).wait_send())
    each(1, 16, lambda d: t_copy(d, z).wait_send())
    each(1, 16, lambda d: x_copy(d, i).wait_send())
    each(1, 16, lambda d: h_copy(d, i).wait_send())
    for n in range(3):
        each(1, 16, lambda d: k_copy(n, d, i).wait_send())
        k_pair(n, c).wait_send()
    for s in range(8):
        ring(s, True).wait_send()
        if s < 7:
            ring(s, False).wait_send()
    each(0, 16, lambda k: pair(k, c).wait_send())
    z_pair(c).wait_send()
    t_pair(c).wait_send()


def on_device(factors):
    vm = pl.BlockSpec(memory_space=pltpu.VMEM)
    dma = pltpu.SemaphoreType.DMA
    v = pltpu.VMEM
    out = pl.pallas_call(
        kernel,
        out_shape=jax.ShapeDtypeStruct((512, 256), F32),
        in_specs=[vm],
        out_specs=vm,
        scratch_shapes=[
            v((2, 16, 2, 16, 1024), F32), v((2, 16, 2, 16, 256), F32), v((2, 16, 2, 16, 512), F32),
            v((16, 2, 16, 128), F32), v((16, 2, 1, 128), F32), v((16, 1, 128), F32),
            v((NB, NB), F32), v((4, NB, 3 * NB), BF16), v((PS, PS), BF16), v((PS, PS), BF16), v((PS, PS), BF16), v((PS, PS), BF16),
            v((PS, PS), F32), v((PS, RW), F32), v((PS, RW), BF16), v((PS, RW), BF16),
            v((PS, 768), BF16), v((PS, 768), BF16), v((PS, 512), F32), v((PS, 512), F32), v((NB, NB), F32),
            dma((16,)), dma((16,)), dma((4,)), dma((16,)), dma((16,)), dma((16,)), dma((16,)),
            dma((3, 16)), dma((3, 16)), dma((6,)), dma((16,)), dma((16,)), dma((16,)), dma((16,)),
            dma((16,)), dma((16,)),
        ],
        compiler_params=pltpu.CompilerParams(
            collective_id=0, has_side_effects=True, vmem_limit_bytes=56 * 1024 * 1024),
        name="refresh",
    )(factors[0])
    return out[None]


def solution(mesh):
    placed = P(None, "row", "col")
    return jax.shard_map(on_device, mesh=mesh, in_specs=(placed,), out_specs=placed, check_vma=False)
```

```python
import jax
import jax.numpy as jnp
from jax import lax
from jax.experimental import pallas as pl
from jax.experimental.pallas import tpu as pltpu
from jax.sharding import PartitionSpec as P

F32, BF16 = jnp.float32, jnp.bfloat16
MESH = pl.DeviceIdType.MESH
damping_share = 0.03162277660168379
NB = 128
MINI = 32
PS = 512
RW = PS + 256 + 512


def split3(x):
    h = x.astype(BF16)
    r = x - h.astype(F32)
    m = r.astype(BF16)
    return h, m, (r - m.astype(F32)).astype(BF16)


def split2(x):
    h = x.astype(BF16)
    return h, (x - h.astype(F32)).astype(BF16)


def tn(a, b):
    return lax.dot_general(a, b, (((0,), (0,)), ((), ())), preferred_element_type=F32)


def nn(a, b):
    return lax.dot_general(a, b, (((1,), (0,)), ((), ())), preferred_element_type=F32)


def left3(h, l):
    return jnp.concatenate([h, l, h], axis=1)


def right3(h, l):
    return jnp.concatenate([h, h, l], axis=0)


def block_inverse(M, b=MINI):
    n = 128
    H = b // 8
    sub = lax.broadcasted_iota(jnp.int32, (8, n), 0)
    lane = lax.broadcasted_iota(jnp.int32, (8, n), 1)
    M = [M[8 * i:8 * i + 8, :] for i in range(n // 8)]
    for s in range(n // b):
        r0 = s * b
        q0 = r0 // 8
        S = [[None] * b for _ in range(H)]
        for k in range(b):
            for h in range(k // 8, H):
                S[h][k] = jnp.broadcast_to(M[q0 + h][:, r0 + k:r0 + k + 1], (8, n))
        inblk = (lane >= r0) & (lane < r0 + b)
        N = [jnp.where(inblk, jnp.where(lane - r0 == sub + 8 * h, 1.0, 0.0).astype(F32), M[q0 + h]) for h in range(H)]
        scale = [None] * H
        d = jnp.broadcast_to(S[0][0][0:1, :], (8, n))
        for j in range(b):
            hj, sj = j // 8, j % 8
            rs = lax.rsqrt(d)
            scale[hj] = rs if sj == 0 else jnp.where(sub == sj, rs, scale[hj])
            if j == b - 1:
                break
            row = [None] * b
            for k in range(j + 1, b):
                row[k] = jnp.broadcast_to(S[k // 8][j][k % 8 : k % 8 + 1, :], (8, n))
            rinv = rs * rs
            hn, sn = (j + 1) // 8, (j + 1) % 8
            d = jnp.broadcast_to(S[hn][j + 1][sn : sn + 1, :], (8, n)) - (row[j + 1] * row[j + 1]) * rinv
            u = [S[h][j] * rinv if h >= hj else None for h in range(H)]
            for k in range(j + 1, b):
                for h in range(k // 8, H):
                    S[h][k] = S[h][k] - u[h] * row[k]
            prow = jnp.broadcast_to(N[hj][sj : sj + 1, :], (8, n))
            for h in range(hj, H):
                if h > hj:
                    N[h] = N[h] - u[h] * prow
                elif sj < 7:
                    N[h] = N[h] - jnp.where(sub > sj, u[h], 0.0) * prow
        Y = jnp.concatenate([N[h] * scale[h] for h in range(H)], axis=0)
        lb = lax.broadcasted_iota(jnp.int32, (b, n), 1)
        for h in range(H):
            M[q0 + h] = Y[8 * h:8 * h + 8, :] if s == n // b - 1 else jnp.where(lane < r0 + b, Y[8 * h:8 * h + 8, :], 0.0)
        if s < n // b - 1:
            h_, m_, l_ = split3(Y)
            R = tn(jnp.concatenate([h_, h_, m_, h_, l_, m_], 0), jnp.concatenate([h_, m_, h_, l_, h_, m_], 0))
            for q in range(q0 + H, n // 8):
                M[q] = jnp.where(inblk, 0.0, M[q]) - R[8 * q:8 * q + 8, :]
    return jnp.concatenate(M, axis=0)

def kernel(a_ref, out_ref, akk, bc, br, zb, tz, tx, dn, wst, lh, ll, kh, kl, g0, g1, ph, pm, qh, ql, y0, y1, w_ref,
           zs, zr, zd, ts, tr, xs, xr, ks, kr, kd, hs, hr, us, ur, ds, dr):
    i = lax.axis_index("row")
    j = lax.axis_index("col")
    z = j // 2
    c = lax.rem(j, 2)
    partner = (i, 2 * z + 1 - c)

    def zpeer(d):
        return (i, 2 * lax.rem(z + d, 16) + c)

    def xpeer(d):
        return (lax.rem(i + d, 16), j)

    def copy(src, dst, ssem, rsem, dev):
        return pltpu.make_async_remote_copy(
            src_ref=src, dst_ref=dst, send_sem=ssem, recv_sem=rsem, device_id=dev, device_id_type=MESH)

    def each(lo, hi, f):
        def step(d, carry):
            f(d)
            return carry
        lax.fori_loop(lo, hi, step, 0)

    barrier = pltpu.get_barrier_semaphore()

    def greet(d):
        pl.semaphore_signal(barrier, inc=1, device_id=zpeer(d), device_id_type=MESH)
        pl.semaphore_signal(barrier, inc=1, device_id=xpeer(d), device_id_type=MESH)

    each(1, 16, greet)
    pl.semaphore_signal(barrier, inc=1, device_id=partner, device_id_type=MESH)

    T = a_ref[:, 0:128].T
    br[0, z, c] = T[0:16, :]
    br[1, z, c] = T[16:32, :]
    lane = lax.broadcasted_iota(jnp.int32, (16, 128), 1)
    p0, p1 = T[0:16, 0:128], T[0:16, 256:384]
    p2, p3 = T[16:32, 0:128], T[16:32, 256:384]
    zb[z, c] = jnp.where(
        lane < 32, p0,
        jnp.where(lane < 64, pltpu.roll(p1, 32, 1), jnp.where(lane < 96, pltpu.roll(p2, 64, 1), pltpu.roll(p3, 96, 1))))
    r = lax.broadcasted_iota(jnp.int32, (512, 256), 0)
    q = lax.broadcasted_iota(jnp.int32, (512, 256), 1)
    on_diagonal = r + 512 * i == q + 256 * j
    t = jnp.sum(jnp.where(on_diagonal, a_ref[...], 0.0), axis=0, keepdims=True)
    tz[z, c] = jnp.broadcast_to(jnp.sum(t, axis=1, keepdims=True), (1, 128))
    for p in range(2):
        for h in range(2):
            bc[p, i, h] = a_ref[256 * h + 16 * p : 256 * h + 16 * p + 16, :]

    pl.semaphore_wait(barrier, 31)

    def behind(v, d):
        return lax.rem(v + 16 - d, 16)

    def z_copy(d, s):
        return copy(zb.at[s, c], zb.at[s, c], zs.at[d], zr.at[d], zpeer(d))

    def t_copy(d, s):
        return copy(tz.at[s, c], tz.at[s, c], ts.at[d], tr.at[d], zpeer(d))

    def x_copy(d, s):
        return copy(bc.at[:, s], bc.at[:, s], xs.at[d], xr.at[d], xpeer(d))

    def h_copy(d, s):
        return copy(tx.at[s], tx.at[s], hs.at[d], hr.at[d], xpeer(d))

    def strip(n, s, h):
        return (akk.at[0, s, h, :, pl.ds(0, 512)], akk.at[0, s, h, :, pl.ds(512, 512)],
                akk.at[1, s, h, :, pl.ds(512, 512)])[n]

    def k_copy(n, d, s):
        return copy(strip(n, s, c), strip(n, s, c), ks.at[n, d], kr.at[n, d], xpeer(d))

    def k_pair(n, h):
        v = (akk.at[0, :, h, :, pl.ds(0, 512)], akk.at[0, :, h, :, pl.ds(512, 512)],
             akk.at[1, :, h, :, pl.ds(512, 512)])[n]
        return copy(v, v, kd.at[n], kd.at[3 + n], partner)

    def z_pair(h):
        return copy(zb.at[:, h], zb.at[:, h], zd.at[0], zd.at[1], partner)

    def t_pair(h):
        return copy(tz.at[:, h], tz.at[:, h], zd.at[2], zd.at[3], partner)

    up_to = (i, 2 * lax.rem(z + 1, 16) + c)
    down_to = (i, 2 * lax.rem(z + 15, 16) + c)

    def ring(s, up, arriving=False):
        e = s + 1 if arriving else s
        k = behind(z, e) if up else lax.rem(z + e, 16)
        o = 0 if up else 8
        return copy(br.at[:, k, c], br.at[:, k, c], us.at[s + o], ur.at[s + o], up_to if up else down_to)

    def pair(k, h):
        return copy(br.at[:, k, h], br.at[:, k, h], ds.at[k], dr.at[k], partner)

    def ring_step(s):
        ring(s - 1, True, True).wait_recv()
        ring(s, True).start()
        pair(behind(z, s), c).start()
        ring(s - 1, False, True).wait_recv()
        if s < 7:
            ring(s, False).start()
        pair(lax.rem(z + s, 16), c).start()

    each(1, 16, lambda d: z_copy(d, z).start())
    each(1, 16, lambda d: t_copy(d, z).start())
    ring(0, True).start()
    ring(0, False).start()
    pair(z, c).start()
    each(1, 16, lambda d: x_copy(d, i).start())
    ring_step(1)
    ring_step(2)
    each(1, 16, lambda d: t_copy(d, behind(z, d)).wait_recv())
    t_pair(c).start()
    each(1, 16, lambda d: z_copy(d, behind(z, d)).wait_recv())
    z_pair(c).start()
    ring_step(3)
    t_pair(1 - c).wait_recv()
    tx[i] = jnp.sum(tz[...].reshape(32, 1, 128), axis=0)
    each(1, 16, lambda d: h_copy(d, i).start())
    z_pair(1 - c).wait_recv()
    S = zb[...].reshape(512, 128).T
    akk[0, i, c, :, 0:512] = jnp.where(c == 0, S[0:16, :], S[32:48, :])
    each(1, 16, lambda d: k_copy(0, d, i).start())
    akk[0, i, c, :, 512:1024] = jnp.where(c == 0, S[64:80, :], S[96:112, :])
    akk[1, i, c, :, 512:1024] = jnp.where(c == 0, S[80:96, :], S[112:128, :])
    ring_step(4)
    each(1, 16, lambda d: h_copy(d, behind(i, d)).wait_recv())
    damp = jnp.sum(tx[...], axis=0) * (damping_share / 8192.0)
    ring_step(5)
    each(1, 16, lambda d: k_copy(0, d, behind(i, d)).wait_recv())
    k_pair(0, c).start()
    each(1, 16, lambda d: k_copy(1, d, i).start())
    each(1, 16, lambda d: k_copy(2, d, i).start())
    k_pair(0, 1 - c).wait_recv()

    damp2 = jnp.concatenate([damp, damp], axis=1)
    damp4 = jnp.concatenate([damp2, damp2], axis=1)
    eye = lax.broadcasted_iota(jnp.int32, (NB, NB), 0) == lax.broadcasted_iota(jnp.int32, (NB, NB), 1)
    deye = jnp.where(eye, damp, 0.0)
    ln = lax.broadcasted_iota(jnp.int32, (PS, 512), 1)
    posl = jnp.where(ln % 256 < 32, (ln % 256 // 16) * 512 + (2 * i + ln // 256) * 16 + ln % 16, -1)
    posr = lax.broadcasted_iota(jnp.int32, (PS, 512), 0)

    g0[...] = akk[0, :, :, :, 0:512].reshape(512, 512)
    dn[...] = g0[0:NB, 0:NB]

    def middle():
        each(1, 16, lambda d: k_copy(1, d, behind(i, d)).wait_recv())
        k_pair(1, c).start()
        each(1, 16, lambda d: x_copy(d, behind(i, d)).wait_recv())
        each(1, 16, lambda d: k_copy(2, d, behind(i, d)).wait_recv())
        k_pair(2, c).start()
        each(0, 16, lambda k: pair(k, 1 - c).wait_recv())
        k_pair(1, 1 - c).wait_recv()
        k_pair(2, 1 - c).wait_recv()
        for b in range(4):
            o = b * NB
            rows = slice(o, o + NB)
            acc = jnp.concatenate([
                akk[0, 4 * b : 4 * b + 4, :, :, 512:1024].reshape(NB, 512),
                bc[0, 4 * b : 4 * b + 4].reshape(NB, 256),
                br[0, 4 * b : 4 * b + 4].reshape(NB, 512) + jnp.where(posr[rows] == posl[rows], damp4, 0.0)], axis=1)
            if b:
                acc = acc - nn(
                    jnp.concatenate([lh[rows, 0:o], ll[rows, 0:o], lh[rows, 0:o]], axis=1),
                    jnp.concatenate([ph[0:o, :], ph[0:o, :], pm[0:o, :]], axis=0))
            Y = nn(wst[b], right3(*split2(acc)))
            y0[rows, :] = Y[:, PS + 256 :]
            ph[rows, :], pm[rows, :] = split2(Y)
            th, tl = split2(Y[:, 0:PS].T)
            kh[:, o : o + NB] = th
            kl[:, o : o + NB] = tl
        left = jnp.concatenate([kh[...], kl[...], kh[...]], axis=1)
        for o in range(0, RW, 256):
            R = nn(left, jnp.concatenate([ph[:, o : o + 256], ph[:, o : o + 256], pm[:, o : o + 256]], axis=0))
            if o < PS:
                src = akk[1, :, :, :, 512 + o : 768 + o].reshape(512, 256)
            elif o == PS:
                src = bc[1].reshape(512, 256)
            else:
                v = o - PS - 256
                src = br[1, :, :, :, v : v + 256].reshape(512, 256) + jnp.where(
                    posr[:, v : v + 256] + 512 == posl[:, v : v + 256], damp2, 0.0)
            g1[:, o : o + 256] = src - R
        dn[...] = g1[0:NB, 0:NB]

    def body(b, carry):
        w_ref[...] = block_inverse(dn[...] + deye)
        for k in range(8):

            @pl.when(b == k)
            def _():
                wl = left3(*split2(w_ref[...]))
                kk = k % 4
                lo = (kk + 1) * NB
                rows = slice(kk * NB, lo)
                if k < 4:
                    wst[k] = wl
                    if k < 2:
                        ring_step(6 + k)
                    if k == 2:
                        ring(7, True, True).wait_recv()
                        pair(lax.rem(z + 8, 16), c).start()
                    if k == 3:
                        middle()
                        return
                    g, hi = g0, PS
                else:
                    g, hi = g1, RW
                Y = nn(wl, right3(*split2(g[rows, lo:hi])))
                h, l = split2(Y)
                if k >= 4:
                    y1[rows, :] = Y[:, PS + 256 - lo :]
                    qh[rows, :] = h[:, PS - lo :]
                    ql[rows, :] = l[:, PS - lo :]
                if kk < 3:
                    th, tl = split2(Y[:, 0 : PS - lo].T)
                    if k < 4:
                        lh[lo:PS, rows] = th
                        ll[lo:PS, rows] = tl
                    left = left3(th, tl)
                    right = right3(h, l)
                    for o in range(0, hi - lo, 256):
                        e = min(o + 256, hi - lo)
                        g[lo:PS, lo + o : lo + e] = g[lo:PS, lo + o : lo + e] - nn(left, right[:, o:e])
                    dn[...] = g[lo : lo + NB, lo : lo + NB]
        return carry

    lax.fori_loop(0, 8, body, 0)

    U = jnp.zeros((512, 256), F32)
    for y, yh, yl, o in ((y0, ph, pm, PS), (y1, qh, ql, 0)):
        th, tl = split2(y[...].T)
        U = U + nn(left3(th, tl), right3(yh[:, o : o + 256], yl[:, o : o + 256]))
    at = pl.ds(pl.multiple_of(j * 16, 16), 16)
    cols = jnp.concatenate([y0[at, :], y1[at, :], jnp.zeros((96, 512), F32)], 0).T
    rm = r % 256
    posrow = jnp.where(rm < 32, (rm // 16) * 512 + (2 * i + r // 256) * 16 + rm % 16, 1024)
    poscol = (q // 16) * 512 + j * 16 + q % 16
    A = a_ref[...] + jnp.where(on_diagonal, damp2, 0.0)
    cols = jnp.concatenate([cols, jnp.zeros((512, 128), F32)], 1)
    out_ref[...] = jnp.where(
        q >= 32, jnp.where(rm >= 32, A - U, 0.0), jnp.where(posrow >= poscol, cols, 0.0))

    each(1, 16, lambda d: z_copy(d, z).wait_send())
    each(1, 16, lambda d: t_copy(d, z).wait_send())
    each(1, 16, lambda d: x_copy(d, i).wait_send())
    each(1, 16, lambda d: h_copy(d, i).wait_send())
    for n in range(3):
        each(1, 16, lambda d: k_copy(n, d, i).wait_send())
        k_pair(n, c).wait_send()
    for s in range(8):
        ring(s, True).wait_send()
        if s < 7:
            ring(s, False).wait_send()
    each(0, 16, lambda k: pair(k, c).wait_send())
    z_pair(c).wait_send()
    t_pair(c).wait_send()


def on_device(factors):
    vm = pl.BlockSpec(memory_space=pltpu.VMEM)
    dma = pltpu.SemaphoreType.DMA
    v = pltpu.VMEM
    out = pl.pallas_call(
        kernel,
        out_shape=jax.ShapeDtypeStruct((512, 256), F32),
        in_specs=[vm],
        out_specs=vm,
        scratch_shapes=[
            v((2, 16, 2, 16, 1024), F32), v((2, 16, 2, 16, 256), F32), v((2, 16, 2, 16, 512), F32),
            v((16, 2, 16, 128), F32), v((16, 2, 1, 128), F32), v((16, 1, 128), F32),
            v((NB, NB), F32), v((4, NB, 3 * NB), BF16), v((PS, PS), BF16), v((PS, PS), BF16), v((PS, PS), BF16), v((PS, PS), BF16),
            v((PS, PS), F32), v((PS, RW), F32), v((PS, RW), BF16), v((PS, RW), BF16),
            v((PS, 768), BF16), v((PS, 768), BF16), v((PS, 512), F32), v((PS, 512), F32), v((NB, NB), F32),
            dma((16,)), dma((16,)), dma((4,)), dma((16,)), dma((16,)), dma((16,)), dma((16,)),
            dma((3, 16)), dma((3, 16)), dma((6,)), dma((16,)), dma((16,)), dma((16,)), dma((16,)),
            dma((16,)), dma((16,)),
        ],
        compiler_params=pltpu.CompilerParams(
            collective_id=0, has_side_effects=True, vmem_limit_bytes=56 * 1024 * 1024),
        name="refresh",
    )(factors[0])
    return out[None]


def solution(mesh):
    placed = P(None, "row", "col")
    return jax.shard_map(on_device, mesh=mesh, in_specs=(placed,), out_specs=placed, check_vma=False)
```

```python
import jax
import jax.numpy as jnp
from jax import lax
from jax.experimental import pallas as pl
from jax.experimental.pallas import tpu as pltpu
from jax.sharding import PartitionSpec as P

F32, BF16 = jnp.float32, jnp.bfloat16
MESH = pl.DeviceIdType.MESH
damping_share = 0.03162277660168379
NB = 128
MINI = 64
AHEAD = (5, 6, 8)
PS = 512
RW = PS + 256 + 512


def split3(x):
    h = x.astype(BF16)
    r = x - h.astype(F32)
    m = r.astype(BF16)
    return h, m, (r - m.astype(F32)).astype(BF16)


def split2(x):
    h = x.astype(BF16)
    return h, (x - h.astype(F32)).astype(BF16)


def tn(a, b):
    return lax.dot_general(a, b, (((0,), (0,)), ((), ())), preferred_element_type=F32)


def nn(a, b):
    return lax.dot_general(a, b, (((1,), (0,)), ((), ())), preferred_element_type=F32)


def left3(h, l):
    return jnp.concatenate([h, l, h], axis=1)


def right3(h, l):
    return jnp.concatenate([h, h, l], axis=0)


def block_inverse(M, b=MINI, ahead=AHEAD):
    n = NB
    H = b // 8
    sub = lax.broadcasted_iota(jnp.int32, (8, n), 0)
    lane = lax.broadcasted_iota(jnp.int32, (8, n), 1)

    def spread(x, s):
        return jnp.broadcast_to(x[s : s + 1, :], (8, n))

    M = [M[8 * q : 8 * q + 8, :] for q in range(n // 8)]
    for r0 in range(0, n, b):
        q0 = r0 // 8
        N = M[q0 : q0 + H]

        def column(k):
            return [
                jnp.broadcast_to(N[h][:, r0 + k : r0 + k + 1], (8, n)) if h >= k // 8 else None for h in range(H)]

        S = {k: column(k) for k in range(ahead[0])}
        have = ahead[0]
        scale = [None] * H
        d = spread(S[0][0], 0)
        for j in range(b):
            hj, sj = j // 8, j % 8
            rs = lax.rsqrt(d)
            scale[hj] = rs if sj == 0 else jnp.where(sub == sj, rs, scale[hj])
            here = lane == r0 + j
            N[hj] = jnp.where(here, jnp.where(sub == sj, 1.0, 0.0), N[hj])
            if j == b - 1:
                break
            C = S.pop(j)
            row = {k: spread(C[k // 8], k % 8) for k in S}
            rinv = rs * rs
            hn, sn = (j + 1) // 8, (j + 1) % 8
            d = spread(S[j + 1][hn], sn) - (row[j + 1] * row[j + 1]) * rinv
            u = [C[h] * rinv if h >= hj else None for h in range(H)]
            for k in S:
                S[k] = [S[k][h] - u[h] * row[k] if h >= k // 8 else None for h in range(H)]
            prow = spread(N[hj], sj)
            for h in range(hj, H):
                if h > hj:
                    N[h] = jnp.where(here, 0.0, N[h]) - u[h] * prow
                elif sj < 7:
                    N[h] = N[h] - jnp.where(sub > sj, u[h], 0.0) * prow
            while have < min(b, j + 1 + ahead[3 * j // b]):
                S[have] = column(have)
                have += 1
        N = [N[h] * scale[h] for h in range(H)]
        for h in range(H):
            M[q0 + h] = jnp.where(lane <= sub + (r0 + 8 * h), N[h], 0.0)
        if r0 + b < n:
            X = [
                jnp.where((lane > sub + (r0 + 8 * h)) & (lane < r0 + b), 0.0, N[h]) for h in range(H)]
            h_, m_, l_ = split3(jnp.concatenate(X, axis=0))
            R = tn(jnp.concatenate([h_, h_, m_, h_, l_, m_], 0), jnp.concatenate([h_, m_, h_, l_, h_, m_], 0))
            inblk = (lane >= r0) & (lane < r0 + b)
            for q in range(q0 + H, n // 8):
                M[q] = jnp.where(inblk, 0.0, M[q]) - R[8 * q : 8 * q + 8, :]
    return jnp.concatenate(M, axis=0)


def kernel(a_ref, out_ref, akk, bc, br, zb, tz, tx, dn, wst, lh, ll, kh, kl, g0, g1, ph, pm, qh, ql, y0, y1, w_ref,
           zs, zr, zd, ts, tr, xs, xr, ks, kr, kd, hs, hr, us, ur, ds, dr):
    i = lax.axis_index("row")
    j = lax.axis_index("col")
    z = j // 2
    c = lax.rem(j, 2)
    partner = (i, 2 * z + 1 - c)

    def zpeer(d):
        return (i, 2 * lax.rem(z + d, 16) + c)

    def xpeer(d):
        return (lax.rem(i + d, 16), j)

    def copy(src, dst, ssem, rsem, dev):
        return pltpu.make_async_remote_copy(
            src_ref=src, dst_ref=dst, send_sem=ssem, recv_sem=rsem, device_id=dev, device_id_type=MESH)

    def each(lo, hi, f):
        def step(d, carry):
            f(d)
            return carry
        lax.fori_loop(lo, hi, step, 0)

    barrier = pltpu.get_barrier_semaphore()

    def greet(d):
        pl.semaphore_signal(barrier, inc=1, device_id=zpeer(d), device_id_type=MESH)
        pl.semaphore_signal(barrier, inc=1, device_id=xpeer(d), device_id_type=MESH)

    each(1, 16, greet)
    pl.semaphore_signal(barrier, inc=1, device_id=partner, device_id_type=MESH)

    T = a_ref[:, 0:128].T
    br[0, z, c] = T[0:16, :]
    br[1, z, c] = T[16:32, :]
    lane = lax.broadcasted_iota(jnp.int32, (16, 128), 1)
    p0, p1 = T[0:16, 0:128], T[0:16, 256:384]
    p2, p3 = T[16:32, 0:128], T[16:32, 256:384]
    zb[z, c] = jnp.where(
        lane < 32, p0,
        jnp.where(lane < 64, pltpu.roll(p1, 32, 1), jnp.where(lane < 96, pltpu.roll(p2, 64, 1), pltpu.roll(p3, 96, 1))))
    r = lax.broadcasted_iota(jnp.int32, (512, 256), 0)
    q = lax.broadcasted_iota(jnp.int32, (512, 256), 1)
    on_diagonal = r + 512 * i == q + 256 * j
    t = jnp.sum(jnp.where(on_diagonal, a_ref[...], 0.0), axis=0, keepdims=True)
    tz[z, c] = jnp.broadcast_to(jnp.sum(t, axis=1, keepdims=True), (1, 128))
    for p in range(2):
        for h in range(2):
            bc[p, i, h] = a_ref[256 * h + 16 * p : 256 * h + 16 * p + 16, :]

    pl.semaphore_wait(barrier, 31)

    def behind(v, d):
        return lax.rem(v + 16 - d, 16)

    def z_copy(d, s):
        return copy(zb.at[s, c], zb.at[s, c], zs.at[d], zr.at[d], zpeer(d))

    def t_copy(d, s):
        return copy(tz.at[s, c], tz.at[s, c], ts.at[d], tr.at[d], zpeer(d))

    def x_copy(d, s):
        return copy(bc.at[:, s], bc.at[:, s], xs.at[d], xr.at[d], xpeer(d))

    def h_copy(d, s):
        return copy(tx.at[s], tx.at[s], hs.at[d], hr.at[d], xpeer(d))

    def lanes(n, x):
        return pl.ds(512, 512) if n == 1 else pl.ds((512 if n else 0) + NB * x, 512 - NB * x)

    def k_send(n, x, d):
        v = akk.at[n // 2, i, c, :, lanes(n, x)]
        return copy(v, v, ks.at[n, d], kr.at[n, i], xpeer(d))

    def k_sends(n, f):
        for x in range(1 if n == 1 else 4):
            if n == 1:
                each(1, 16, lambda d: f(k_send(n, x, d)))
            else:

                @pl.when(i // 4 == x)
                def _():
                    each(1, 16, lambda d: f(k_send(n, x, d)))

    def k_recv(n):
        for x in range(4):

            def one(s, carry):
                @pl.when(s != i)
                def _():
                    v = akk.at[n // 2, s, c, :, lanes(n, x)]
                    copy(v, v, ks.at[n, 0], kr.at[n, s], partner).wait_recv()
                return carry

            lax.fori_loop(4 * x, 4 * x + 4, one, 0)

    def k_pair(n, x, h):
        v = akk.at[n // 2, pl.ds(4 * x, 4), h, :, lanes(n, x)]
        return copy(v, v, kd.at[0, n, x], kd.at[1, n, x], partner)

    def k_pairs(n, h, f):
        for x in range(4):
            f(k_pair(n, x, h))

    def begin(v):
        v.start()

    def arrived(v):
        v.wait_recv()

    def left(v):
        v.wait_send()

    def z_pair(h):
        return copy(zb.at[:, h], zb.at[:, h], zd.at[0], zd.at[1], partner)

    def t_pair(h):
        return copy(tz.at[:, h], tz.at[:, h], zd.at[2], zd.at[3], partner)

    up_to = (i, 2 * lax.rem(z + 1, 16) + c)
    down_to = (i, 2 * lax.rem(z + 15, 16) + c)

    def ring(s, up, arriving=False):
        e = s + 1 if arriving else s
        k = behind(z, e) if up else lax.rem(z + e, 16)
        o = 0 if up else 8
        return copy(br.at[:, k, c], br.at[:, k, c], us.at[s + o], ur.at[s + o], up_to if up else down_to)

    def pair(k, h):
        return copy(br.at[:, k, h], br.at[:, k, h], ds.at[k], dr.at[k], partner)

    def ring_step(s):
        ring(s - 1, True, True).wait_recv()
        ring(s, True).start()
        pair(behind(z, s), c).start()
        ring(s - 1, False, True).wait_recv()
        if s < 7:
            ring(s, False).start()
        pair(lax.rem(z + s, 16), c).start()

    each(1, 16, lambda d: z_copy(d, z).start())
    each(1, 16, lambda d: t_copy(d, z).start())
    ring(0, True).start()
    ring(0, False).start()
    pair(z, c).start()
    each(1, 16, lambda d: x_copy(d, i).start())
    each(1, 16, lambda d: t_copy(d, behind(z, d)).wait_recv())
    t_pair(c).start()
    each(1, 16, lambda d: z_copy(d, behind(z, d)).wait_recv())
    z_pair(c).start()
    ring_step(1)
    t_pair(1 - c).wait_recv()
    tx[i] = jnp.sum(tz[...].reshape(32, 1, 128), axis=0)
    each(1, 16, lambda d: h_copy(d, i).start())
    z_pair(1 - c).wait_recv()
    S = zb[...].reshape(512, 128).T
    akk[0, i, c, :, 0:512] = jnp.where(c == 0, S[0:16, :], S[32:48, :])
    k_sends(0, begin)
    akk[0, i, c, :, 512:1024] = jnp.where(c == 0, S[64:80, :], S[96:112, :])
    akk[1, i, c, :, 512:1024] = jnp.where(c == 0, S[80:96, :], S[112:128, :])
    ring_step(2)
    each(1, 16, lambda d: h_copy(d, behind(i, d)).wait_recv())
    damp = jnp.sum(tx[...], axis=0) * (damping_share / 8192.0)
    ring_step(3)
    k_recv(0)
    k_pairs(0, c, begin)
    k_sends(1, begin)
    k_sends(2, begin)
    ring_step(4)
    k_pairs(0, 1 - c, arrived)

    damp2 = jnp.concatenate([damp, damp], axis=1)
    damp4 = jnp.concatenate([damp2, damp2], axis=1)
    eye = lax.broadcasted_iota(jnp.int32, (NB, NB), 0) == lax.broadcasted_iota(jnp.int32, (NB, NB), 1)
    deye = jnp.where(eye, damp, 0.0)
    ln = lax.broadcasted_iota(jnp.int32, (PS, 512), 1)
    posl = jnp.where(ln % 256 < 32, (ln % 256 // 16) * 512 + (2 * i + ln // 256) * 16 + ln % 16, -1)
    posr = lax.broadcasted_iota(jnp.int32, (PS, 512), 0)

    g0[...] = akk[0, :, :, :, 0:512].reshape(512, 512)
    dn[...] = g0[0:NB, 0:NB]

    def middle():
        ring(7, True, True).wait_recv()
        pair(lax.rem(z + 8, 16), c).start()
        each(1, 16, lambda d: x_copy(d, behind(i, d)).wait_recv())
        k_pairs(1, 1 - c, arrived)
        k_pairs(2, 1 - c, arrived)
        each(0, 16, lambda k: pair(k, 1 - c).wait_recv())
        for b in range(4):
            o = b * NB
            rows = slice(o, o + NB)
            acc = jnp.concatenate([
                akk[0, 4 * b : 4 * b + 4, :, :, 512:1024].reshape(NB, 512),
                bc[0, 4 * b : 4 * b + 4].reshape(NB, 256),
                br[0, 4 * b : 4 * b + 4].reshape(NB, 512) + jnp.where(posr[rows] == posl[rows], damp4, 0.0)], axis=1)
            if b:
                acc = acc - nn(
                    jnp.concatenate([lh[rows, 0:o], ll[rows, 0:o], lh[rows, 0:o]], axis=1),
                    jnp.concatenate([ph[0:o, :], ph[0:o, :], pm[0:o, :]], axis=0))
            Y = nn(wst[b], right3(*split2(acc)))
            y0[rows, :] = Y[:, PS + 256 :]
            ph[rows, :], pm[rows, :] = split2(Y)
            th, tl = split2(Y[:, 0:PS].T)
            kh[:, o : o + NB] = th
            kl[:, o : o + NB] = tl
        lhs = jnp.concatenate([kh[...], kl[...], kh[...]], axis=1)
        for o in range(0, RW, 256):
            R = nn(lhs, jnp.concatenate([ph[:, o : o + 256], ph[:, o : o + 256], pm[:, o : o + 256]], axis=0))
            if o < PS:
                src = akk[1, :, :, :, 512 + o : 768 + o].reshape(512, 256)
            elif o == PS:
                src = bc[1].reshape(512, 256)
            else:
                v = o - PS - 256
                src = br[1, :, :, :, v : v + 256].reshape(512, 256) + jnp.where(
                    posr[:, v : v + 256] + 512 == posl[:, v : v + 256], damp2, 0.0)
            g1[:, o : o + 256] = src - R
        dn[...] = g1[0:NB, 0:NB]

    def body(b, carry):
        w_ref[...] = block_inverse(dn[...] + deye)
        for k in range(8):

            @pl.when(b == k)
            def _():
                wl = left3(*split2(w_ref[...]))
                kk = k % 4
                lo = (kk + 1) * NB
                rows = slice(kk * NB, lo)
                if k < 4:
                    wst[k] = wl
                    if k < 3:
                        ring_step(5 + k)
                    if k == 2:
                        k_recv(1)
                        k_pairs(1, c, begin)
                        k_recv(2)
                        k_pairs(2, c, begin)
                    if k == 3:
                        middle()
                        return
                    g, hi = g0, PS
                else:
                    g, hi = g1, RW
                Y = nn(wl, right3(*split2(g[rows, lo:hi])))
                h, l = split2(Y)
                if k >= 4:
                    y1[rows, :] = Y[:, PS + 256 - lo :]
                    qh[rows, :] = h[:, PS - lo :]
                    ql[rows, :] = l[:, PS - lo :]
                if kk < 3:
                    th, tl = split2(Y[:, 0 : PS - lo].T)
                    if k < 4:
                        lh[lo:PS, rows] = th
                        ll[lo:PS, rows] = tl
                    lhs = left3(th, tl)
                    right = right3(h, l)
                    for o in range(0, hi - lo, 256):
                        e = min(o + 256, hi - lo)
                        g[lo:PS, lo + o : lo + e] = g[lo:PS, lo + o : lo + e] - nn(lhs, right[:, o:e])
                    dn[...] = g[lo : lo + NB, lo : lo + NB]
        return carry

    lax.fori_loop(0, 8, body, 0)

    U = jnp.zeros((512, 256), F32)
    for y, yh, yl, o in ((y0, ph, pm, PS), (y1, qh, ql, 0)):
        th, tl = split2(y[...].T)
        U = U + nn(left3(th, tl), right3(yh[:, o : o + 256], yl[:, o : o + 256]))
    at = pl.ds(pl.multiple_of(j * 16, 16), 16)
    cols = jnp.concatenate([y0[at, :], y1[at, :], jnp.zeros((96, 512), F32)], 0).T
    rm = r % 256
    posrow = jnp.where(rm < 32, (rm // 16) * 512 + (2 * i + r // 256) * 16 + rm % 16, 1024)
    poscol = (q // 16) * 512 + j * 16 + q % 16
    A = a_ref[...] + jnp.where(on_diagonal, damp2, 0.0)
    cols = jnp.concatenate([cols, jnp.zeros((512, 128), F32)], 1)
    out_ref[...] = jnp.where(
        q >= 32, jnp.where(rm >= 32, A - U, 0.0), jnp.where(posrow >= poscol, cols, 0.0))

    each(1, 16, lambda d: z_copy(d, z).wait_send())
    each(1, 16, lambda d: t_copy(d, z).wait_send())
    each(1, 16, lambda d: x_copy(d, i).wait_send())
    each(1, 16, lambda d: h_copy(d, i).wait_send())
    for n in range(3):
        k_sends(n, left)
        k_pairs(n, c, left)
    for s in range(8):
        ring(s, True).wait_send()
        if s < 7:
            ring(s, False).wait_send()
    each(0, 16, lambda k: pair(k, c).wait_send())
    z_pair(c).wait_send()
    t_pair(c).wait_send()


def on_device(factors):
    vm = pl.BlockSpec(memory_space=pltpu.VMEM)
    dma = pltpu.SemaphoreType.DMA
    v = pltpu.VMEM
    out = pl.pallas_call(
        kernel,
        out_shape=jax.ShapeDtypeStruct((512, 256), F32),
        in_specs=[vm],
        out_specs=vm,
        scratch_shapes=[
            v((2, 16, 2, 16, 1024), F32), v((2, 16, 2, 16, 256), F32), v((2, 16, 2, 16, 512), F32),
            v((16, 2, 16, 128), F32), v((16, 2, 1, 128), F32), v((16, 1, 128), F32),
            v((NB, NB), F32), v((4, NB, 3 * NB), BF16), v((PS, PS), BF16), v((PS, PS), BF16), v((PS, PS), BF16), v((PS, PS), BF16),
            v((PS, PS), F32), v((PS, RW), F32), v((PS, RW), BF16), v((PS, RW), BF16),
            v((PS, 768), BF16), v((PS, 768), BF16), v((PS, 512), F32), v((PS, 512), F32), v((NB, NB), F32),
            dma((16,)), dma((16,)), dma((4,)), dma((16,)), dma((16,)), dma((16,)), dma((16,)),
            dma((3, 16)), dma((3, 16)), dma((2, 3, 4)), dma((16,)), dma((16,)), dma((16,)), dma((16,)),
            dma((16,)), dma((16,)),
        ],
        compiler_params=pltpu.CompilerParams(
            collective_id=0, has_side_effects=True, vmem_limit_bytes=56 * 1024 * 1024),
        name="refresh",
    )(factors[0])
    return out[None]


def solution(mesh):
    placed = P(None, "row", "col")
    return jax.shard_map(on_device, mesh=mesh, in_specs=(placed,), out_specs=placed, check_vma=False)
```

```python
import jax
import jax.numpy as jnp
from jax import lax
from jax.experimental import pallas as pl
from jax.experimental.pallas import tpu as pltpu
from jax.sharding import PartitionSpec as P

F32, BF16 = jnp.float32, jnp.bfloat16
MESH = pl.DeviceIdType.MESH
damping_share = 0.03162277660168379
NB = 128
MINI = 64
AHEAD = (6, 6, 7)
PS = 512
RW = PS + 256 + 512


def split3(x):
    h = x.astype(BF16)
    r = x - h.astype(F32)
    m = r.astype(BF16)
    return h, m, (r - m.astype(F32)).astype(BF16)


def split2(x):
    h = x.astype(BF16)
    return h, (x - h.astype(F32)).astype(BF16)


def tn(a, b):
    return lax.dot_general(a, b, (((0,), (0,)), ((), ())), preferred_element_type=F32)


def nn(a, b):
    return lax.dot_general(a, b, (((1,), (0,)), ((), ())), preferred_element_type=F32)


def left3(h, l):
    return jnp.concatenate([h, l, h], axis=1)


def right3(h, l):
    return jnp.concatenate([h, h, l], axis=0)


def block_inverse(M, b=MINI, ahead=AHEAD):
    n = NB
    H = b // 8
    sub = lax.broadcasted_iota(jnp.int32, (8, n), 0)
    lane = lax.broadcasted_iota(jnp.int32, (8, n), 1)

    def spread(x, s):
        return jnp.broadcast_to(x[s : s + 1, :], (8, n))

    M = [M[8 * q : 8 * q + 8, :] for q in range(n // 8)]
    for r0 in range(0, n, b):
        q0 = r0 // 8
        N = M[q0 : q0 + H]

        def column(k):
            return [
                jnp.broadcast_to(N[h][:, r0 + k : r0 + k + 1], (8, n)) if h >= k // 8 else None for h in range(H)]

        S = {k: column(k) for k in range(ahead[0])}
        have = ahead[0]
        scale = [None] * H
        d = spread(S[0][0], 0)
        for j in range(b):
            hj, sj = j // 8, j % 8
            rs = lax.rsqrt(d)
            scale[hj] = rs if sj == 0 else jnp.where(sub == sj, rs, scale[hj])
            here = lane == r0 + j
            N[hj] = jnp.where(here, jnp.where(sub == sj, 1.0, 0.0), N[hj])
            if j == b - 1:
                break
            C = S.pop(j)
            row = {k: spread(C[k // 8], k % 8) for k in S}
            rinv = rs * rs
            hn, sn = (j + 1) // 8, (j + 1) % 8
            d = spread(S[j + 1][hn], sn) - (row[j + 1] * row[j + 1]) * rinv
            u = [C[h] * rinv if h >= hj else None for h in range(H)]
            for k in S:
                S[k] = [S[k][h] - u[h] * row[k] if h >= k // 8 else None for h in range(H)]
            prow = spread(N[hj], sj)
            for h in range(hj, H):
                if h > hj:
                    N[h] = jnp.where(here, 0.0, N[h]) - u[h] * prow
                elif sj < 7:
                    N[h] = N[h] - jnp.where(sub > sj, u[h], 0.0) * prow
            while have < min(b, j + 1 + ahead[3 * j // b]):
                S[have] = column(have)
                have += 1
        N = [N[h] * scale[h] for h in range(H)]
        for h in range(H):
            M[q0 + h] = jnp.where(lane <= sub + (r0 + 8 * h), N[h], 0.0)
        if r0 + b < n:
            X = [
                jnp.where((lane > sub + (r0 + 8 * h)) & (lane < r0 + b), 0.0, N[h]) for h in range(H)]
            h_, m_, l_ = split3(jnp.concatenate(X, axis=0))
            R = tn(jnp.concatenate([h_, h_, m_, h_, l_, m_], 0), jnp.concatenate([h_, m_, h_, l_, h_, m_], 0))
            inblk = (lane >= r0) & (lane < r0 + b)
            for q in range(q0 + H, n // 8):
                M[q] = jnp.where(inblk, 0.0, M[q]) - R[8 * q : 8 * q + 8, :]
    return jnp.concatenate(M, axis=0)


def kernel(a_ref, yr, yc, damp_ref, akk, bc, br, zb, tz, tx, dn, wst, lh, ll, kh, kl, g0, g1, ph, pm,
           w_ref, zs, zr, zd, vs, vr, ts, tr, xs, xr, ks, kr, kd, hs, hr, us, ur, ds, dr):
    i = lax.axis_index("row")
    j = lax.axis_index("col")
    z = j // 2
    c = lax.rem(j, 2)
    partner = (i, 2 * z + 1 - c)

    def zpeer(d):
        return (i, 2 * lax.rem(z + d, 16) + c)

    def xpeer(d):
        return (lax.rem(i + d, 16), j)

    def copy(src, dst, ssem, rsem, dev):
        return pltpu.make_async_remote_copy(
            src_ref=src, dst_ref=dst, send_sem=ssem, recv_sem=rsem, device_id=dev, device_id_type=MESH)

    def each(lo, hi, f):
        def step(d, carry):
            f(d)
            return carry
        lax.fori_loop(lo, hi, step, 0)

    barrier = pltpu.get_barrier_semaphore()

    def greet(d):
        pl.semaphore_signal(barrier, inc=1, device_id=zpeer(d), device_id_type=MESH)
        pl.semaphore_signal(barrier, inc=1, device_id=xpeer(d), device_id_type=MESH)

    each(1, 16, greet)
    pl.semaphore_signal(barrier, inc=1, device_id=partner, device_id_type=MESH)

    lane = lax.broadcasted_iota(jnp.int32, (32, 128), 1)
    V = jnp.concatenate([a_ref[0:32, 0:128], a_ref[256:288, 0:128], jnp.zeros((64, 128), F32)], 0).T[0:32, :]
    v0 = jnp.where(lane < 16, V, pltpu.roll(V, 112, 1))
    v1 = jnp.where(lane < 16, pltpu.roll(V, 112, 1), pltpu.roll(V, 96, 1))
    part = lane[0:8, :]
    zb[0, z, c] = jnp.where(
        part < 32, v0[0:8, :],
        jnp.where(part < 64, pltpu.roll(v0[8:16, :], 32, 1),
                  jnp.where(part < 96, pltpu.roll(v0[16:24, :], 64, 1), pltpu.roll(v0[24:32, :], 96, 1))))
    zb[1, z, c] = jnp.where(part < 32, v1[16:24, :], pltpu.roll(v1[24:32, :], 32, 1))
    r = lax.broadcasted_iota(jnp.int32, (256, 256), 0)
    q = lax.broadcasted_iota(jnp.int32, (256, 256), 1)
    own = a_ref[pl.ds(pl.multiple_of(256 * c, 256), 256), :]
    t = jnp.sum(jnp.where((r == q) & (z == i), own, 0.0), axis=0, keepdims=True)
    tz[z, c] = jnp.broadcast_to(jnp.sum(t, axis=1, keepdims=True), (1, 128))

    pl.semaphore_wait(barrier, 31)

    def behind(v, d):
        return lax.rem(v + 16 - d, 16)

    def z_copy(d, s):
        return copy(zb.at[0, s, c], zb.at[0, s, c], zs.at[d], zr.at[d], zpeer(d))

    def v_copy(d, s):
        return copy(zb.at[1, s, c], zb.at[1, s, c], vs.at[d], vr.at[d], zpeer(d))

    def t_copy(d, s):
        return copy(tz.at[s, c], tz.at[s, c], ts.at[d], tr.at[d], zpeer(d))

    def x_copy(d, s):
        return copy(bc.at[:, s], bc.at[:, s], xs.at[d], xr.at[d], xpeer(d))

    def h_copy(d, s):
        return copy(tx.at[s], tx.at[s], hs.at[d], hr.at[d], xpeer(d))

    def lanes(n, x):
        return pl.ds(512, 512) if n == 1 else pl.ds((512 if n else 0) + NB * x, 512 - NB * x)

    def k_send(n, x, d):
        v = akk.at[n // 2, i, c, :, lanes(n, x)]
        return copy(v, v, ks.at[n, d], kr.at[n, i], xpeer(d))

    def k_sends(n, f):
        for x in range(1 if n == 1 else 4):
            if n == 1:
                each(1, 16, lambda d: f(k_send(n, x, d)))
            else:

                @pl.when(i // 4 == x)
                def _():
                    each(1, 16, lambda d: f(k_send(n, x, d)))

    def k_recv(n):
        for x in range(4):

            def one(s, carry):
                @pl.when(s != i)
                def _():
                    v = akk.at[n // 2, s, c, :, lanes(n, x)]
                    copy(v, v, ks.at[n, 0], kr.at[n, s], partner).wait_recv()
                return carry

            lax.fori_loop(4 * x, 4 * x + 4, one, 0)

    def k_pair(n, x, h):
        v = akk.at[n // 2, pl.ds(4 * x, 4), h, :, lanes(n, x)]
        return copy(v, v, kd.at[0, n, x], kd.at[1, n, x], partner)

    def k_pairs(n, h, f):
        for x in range(4):
            f(k_pair(n, x, h))

    def begin(v):
        v.start()

    def arrived(v):
        v.wait_recv()

    def left(v):
        v.wait_send()

    def z_pair(h):
        return copy(zb.at[0, :, h], zb.at[0, :, h], zd.at[0], zd.at[1], partner)

    def v_pair(h):
        return copy(zb.at[1, :, h], zb.at[1, :, h], zd.at[4], zd.at[5], partner)

    def t_pair(h):
        return copy(tz.at[:, h], tz.at[:, h], zd.at[2], zd.at[3], partner)

    up_to = (i, 2 * lax.rem(z + 1, 16) + c)
    down_to = (i, 2 * lax.rem(z + 15, 16) + c)

    def ring(s, up, arriving=False):
        e = s + 1 if arriving else s
        k = behind(z, e) if up else lax.rem(z + e, 16)
        o = 0 if up else 8
        return copy(br.at[:, k, c], br.at[:, k, c], us.at[s + o], ur.at[s + o], up_to if up else down_to)

    def pair(k, h):
        return copy(br.at[:, k, h], br.at[:, k, h], ds.at[k], dr.at[k], partner)

    def ring_step(s):
        ring(s - 1, True, True).wait_recv()
        ring(s, True).start()
        pair(behind(z, s), c).start()
        ring(s - 1, False, True).wait_recv()
        if s < 7:
            ring(s, False).start()
        pair(lax.rem(z + s, 16), c).start()

    def assembled(n):
        p = zb[n].reshape(32, 1, 8, 128)
        two = pltpu.roll(p.reshape(256, 128), 96, 1).reshape(32, 1, 8, 128)
        return jnp.concatenate([p, two], axis=1).reshape(512, 128).T

    each(1, 16, lambda d: z_copy(d, z).start())
    each(1, 16, lambda d: t_copy(d, z).start())
    T = a_ref[:, 0:128].T
    br[0, z, c] = T[0:16, :]
    br[1, z, c] = T[16:32, :]
    for p in range(2):
        for h in range(2):
            bc[p, i, h] = a_ref[256 * h + 16 * p : 256 * h + 16 * p + 16, :]
    ring(0, True).start()
    ring(0, False).start()
    each(1, 16, lambda d: v_copy(d, z).start())
    pair(z, c).start()
    each(1, 16, lambda d: x_copy(d, i).start())
    ring_step(1)
    each(1, 16, lambda d: z_copy(d, behind(z, d)).wait_recv())
    z_pair(c).start()
    each(1, 16, lambda d: t_copy(d, behind(z, d)).wait_recv())
    t_pair(c).start()
    ring_step(2)
    z_pair(1 - c).wait_recv()
    S = assembled(0)
    akk[0, i, c, :, 0:512] = jnp.where(c == 0, S[0:16, :], S[16:32, :])
    t_pair(1 - c).wait_recv()
    tx[i] = jnp.sum(tz[...].reshape(32, 1, 128), axis=0)
    each(1, 16, lambda d: h_copy(d, i).start())
    k_sends(0, begin)
    akk[0, i, c, :, 512:1024] = jnp.where(c == 0, S[64:80, :], S[80:96, :])
    ring_step(3)
    each(1, 16, lambda d: v_copy(d, behind(z, d)).wait_recv())
    v_pair(c).start()
    v_pair(1 - c).wait_recv()
    S = assembled(1)
    akk[1, i, c, :, 512:1024] = jnp.where(c == 0, S[0:16, :], S[16:32, :])
    each(1, 16, lambda d: h_copy(d, behind(i, d)).wait_recv())
    damp = jnp.sum(tx[...], axis=0) * (damping_share / 8192.0)
    damp_ref[...] = jnp.broadcast_to(damp, (8, 128))
    ring_step(4)
    k_recv(0)
    k_pairs(0, c, begin)
    k_sends(1, begin)
    k_sends(2, begin)
    k_pairs(0, 1 - c, arrived)

    damp2 = jnp.concatenate([damp, damp], axis=1)
    damp4 = jnp.concatenate([damp2, damp2], axis=1)
    eye = lax.broadcasted_iota(jnp.int32, (NB, NB), 0) == lax.broadcasted_iota(jnp.int32, (NB, NB), 1)
    deye = jnp.where(eye, damp, 0.0)
    ln = lax.broadcasted_iota(jnp.int32, (PS, 512), 1)
    posl = jnp.where(ln % 256 < 32, (ln % 256 // 16) * 512 + (2 * i + ln // 256) * 16 + ln % 16, -1)
    posr = lax.broadcasted_iota(jnp.int32, (PS, 512), 0)

    g0[...] = akk[0, :, :, :, 0:512].reshape(512, 512)
    dn[...] = g0[0:NB, 0:NB]

    def middle():
        ring(7, True, True).wait_recv()
        pair(lax.rem(z + 8, 16), c).start()
        each(1, 16, lambda d: x_copy(d, behind(i, d)).wait_recv())
        k_pairs(1, 1 - c, arrived)
        k_pairs(2, 1 - c, arrived)
        each(0, 16, lambda k: pair(k, 1 - c).wait_recv())
        for b in range(4):
            o = b * NB
            rows = slice(o, o + NB)
            acc = jnp.concatenate([
                akk[0, 4 * b : 4 * b + 4, :, :, 512:1024].reshape(NB, 512),
                bc[0, 4 * b : 4 * b + 4].reshape(NB, 256),
                br[0, 4 * b : 4 * b + 4].reshape(NB, 512) + jnp.where(posr[rows] == posl[rows], damp4, 0.0)], axis=1)
            if b:
                acc = acc - nn(
                    jnp.concatenate([lh[rows, 0:o], ll[rows, 0:o], lh[rows, 0:o]], axis=1),
                    jnp.concatenate([ph[0:o, :], ph[0:o, :], pm[0:o, :]], axis=0))
            Y = nn(wst[b], right3(*split2(acc)))
            yr[rows, :] = Y[:, PS + 256 :]
            yc[rows, :] = Y[:, PS : PS + 256]
            ph[rows, :], pm[rows, :] = split2(Y)
            th, tl = split2(Y[:, 0:PS].T)
            kh[:, o : o + NB] = th
            kl[:, o : o + NB] = tl
        lhs = jnp.concatenate([kh[...], kl[...], kh[...]], axis=1)
        for o in range(0, RW, 256):
            R = nn(lhs, jnp.concatenate([ph[:, o : o + 256], ph[:, o : o + 256], pm[:, o : o + 256]], axis=0))
            if o < PS:
                src = akk[1, :, :, :, 512 + o : 768 + o].reshape(512, 256)
            elif o == PS:
                src = bc[1].reshape(512, 256)
            else:
                v = o - PS - 256
                src = br[1, :, :, :, v : v + 256].reshape(512, 256) + jnp.where(
                    posr[:, v : v + 256] + 512 == posl[:, v : v + 256], damp2, 0.0)
            g1[:, o : o + 256] = src - R
        dn[...] = g1[0:NB, 0:NB]

    def body(b, carry):
        w_ref[...] = block_inverse(dn[...] + deye)
        for k in range(8):

            @pl.when(b == k)
            def _():
                wl = left3(*split2(w_ref[...]))
                kk = k % 4
                lo = (kk + 1) * NB
                rows = slice(kk * NB, lo)
                if k < 4:
                    wst[k] = wl
                    if k < 3:
                        ring_step(5 + k)
                    if k == 2:
                        k_recv(1)
                        k_pairs(1, c, begin)
                        k_recv(2)
                        k_pairs(2, c, begin)
                    if k == 3:
                        middle()
                        return
                    g, hi = g0, PS
                else:
                    g, hi = g1, RW
                Y = nn(wl, right3(*split2(g[rows, lo:hi])))
                h, l = split2(Y)
                if k >= 4:
                    yr[PS + kk * NB : PS + lo, :] = Y[:, PS + 256 - lo :]
                    yc[PS + kk * NB : PS + lo, :] = Y[:, PS - lo : PS + 256 - lo]
                if kk < 3:
                    th, tl = split2(Y[:, 0 : PS - lo].T)
                    if k < 4:
                        lh[lo:PS, rows] = th
                        ll[lo:PS, rows] = tl
                    lhs = left3(th, tl)
                    right = right3(h, l)
                    for o in range(0, hi - lo, 256):
                        e = min(o + 256, hi - lo)
                        g[lo:PS, lo + o : lo + e] = g[lo:PS, lo + o : lo + e] - nn(lhs, right[:, o:e])
                    dn[...] = g[lo : lo + NB, lo : lo + NB]
        return carry

    lax.fori_loop(0, 8, body, 0)

    each(1, 16, lambda d: z_copy(d, z).wait_send())
    each(1, 16, lambda d: v_copy(d, z).wait_send())
    v_pair(c).wait_send()
    each(1, 16, lambda d: t_copy(d, z).wait_send())
    each(1, 16, lambda d: x_copy(d, i).wait_send())
    each(1, 16, lambda d: h_copy(d, i).wait_send())
    for n in range(3):
        k_sends(n, left)
        k_pairs(n, c, left)
    for s in range(8):
        ring(s, True).wait_send()
        if s < 7:
            ring(s, False).wait_send()
    each(0, 16, lambda k: pair(k, c).wait_send())
    z_pair(c).wait_send()
    t_pair(c).wait_send()


def finish(a_ref, yr, yc, damp_ref, out_ref):
    i = lax.axis_index("row")
    j = lax.axis_index("col")
    r = lax.broadcasted_iota(jnp.int32, (512, 256), 0)
    q = lax.broadcasted_iota(jnp.int32, (512, 256), 1)
    U = jnp.zeros((512, 256), F32)
    for o in (0, PS):
        th, tl = split2(yr[o : o + PS, :].T)
        U = U + nn(left3(th, tl), right3(*split2(yc[o : o + PS, :])))
    at = [pl.ds(pl.multiple_of(j * 16 + o, 16), 16) for o in (0, PS)]
    cols = jnp.concatenate([yr[at[0], :], yr[at[1], :], jnp.zeros((96, 512), F32)], 0).T
    rm = r % 256
    posrow = jnp.where(rm < 32, (rm // 16) * 512 + (2 * i + r // 256) * 16 + rm % 16, 1024)
    poscol = (q // 16) * 512 + j * 16 + q % 16
    damp = damp_ref[0:1, :]
    damp2 = jnp.concatenate([damp, damp], axis=1)
    A = a_ref[...] + jnp.where(r + 512 * i == q + 256 * j, damp2, 0.0)
    cols = jnp.concatenate([cols, jnp.zeros((512, 128), F32)], 1)
    out_ref[...] = jnp.where(
        q >= 32, jnp.where(rm >= 32, A - U, 0.0), jnp.where(posrow >= poscol, cols, 0.0))


def on_device(factors):
    vm = pl.BlockSpec(memory_space=pltpu.VMEM)
    dma = pltpu.SemaphoreType.DMA
    v = pltpu.VMEM
    f = jax.ShapeDtypeStruct
    parts = pl.pallas_call(
        kernel,
        out_shape=[f((1024, 512), F32), f((1024, 256), F32), f((8, 128), F32)],
        in_specs=[vm],
        out_specs=[vm] * 3,
        scratch_shapes=[
            v((2, 16, 2, 16, 1024), F32), v((2, 16, 2, 16, 256), F32),
            v((2, 16, 2, 16, 512), F32), v((2, 16, 2, 8, 128), F32), v((16, 2, 1, 128), F32), v((16, 1, 128), F32),
            v((NB, NB), F32), v((4, NB, 3 * NB), BF16), v((PS, PS), BF16), v((PS, PS), BF16), v((PS, PS), BF16),
            v((PS, PS), BF16), v((PS, PS), F32), v((PS, RW), F32), v((PS, RW), BF16), v((PS, RW), BF16),
            v((NB, NB), F32),
            dma((16,)), dma((16,)), dma((6,)), dma((16,)), dma((16,)), dma((16,)), dma((16,)), dma((16,)), dma((16,)),
            dma((3, 16)), dma((3, 16)), dma((2, 3, 4)), dma((16,)), dma((16,)), dma((16,)), dma((16,)),
            dma((16,)), dma((16,)),
        ],
        compiler_params=pltpu.CompilerParams(
            collective_id=0, has_side_effects=True, vmem_limit_bytes=42 * 1024 * 1024),
        name="gather_eliminate",
    )(factors[0])
    out = pl.pallas_call(
        finish,
        out_shape=f((512, 256), F32),
        in_specs=[vm] * 4,
        out_specs=vm,
        compiler_params=pltpu.CompilerParams(vmem_limit_bytes=16 * 1024 * 1024),
        name="finish",
    )(factors[0], *parts)
    return out[None]


def solution(mesh):
    placed = P(None, "row", "col")
    return jax.shard_map(on_device, mesh=mesh, in_specs=(placed,), out_specs=placed, check_vma=False)
```

```python
import jax
import jax.numpy as jnp
from jax import lax
from jax.experimental import pallas as pl
from jax.experimental.pallas import tpu as pltpu
from jax.sharding import PartitionSpec as P

F32, BF16 = jnp.float32, jnp.bfloat16
MESH = pl.DeviceIdType.MESH
damping_share = 0.03162277660168379
NB = 128
MINI = 64
AHEAD = (6, 6, 7)
PS = 512
RW = PS + 256 + 512


def split3(x):
    h = x.astype(BF16)
    r = x - h.astype(F32)
    m = r.astype(BF16)
    return h, m, (r - m.astype(F32)).astype(BF16)


def split2(x):
    h = x.astype(BF16)
    return h, (x - h.astype(F32)).astype(BF16)


def tn(a, b):
    return lax.dot_general(a, b, (((0,), (0,)), ((), ())), preferred_element_type=F32)


def nn(a, b):
    return lax.dot_general(a, b, (((1,), (0,)), ((), ())), preferred_element_type=F32)


def left3(h, l):
    return jnp.concatenate([h, l, h], axis=1)


def right3(h, l):
    return jnp.concatenate([h, h, l], axis=0)


def block_inverse(M, b=MINI, ahead=AHEAD):
    n = NB
    H = b // 8
    sub = lax.broadcasted_iota(jnp.int32, (8, n), 0)
    lane = lax.broadcasted_iota(jnp.int32, (8, n), 1)

    def spread(x, s):
        return jnp.broadcast_to(x[s : s + 1, :], (8, n))

    M = [M[8 * q : 8 * q + 8, :] for q in range(n // 8)]
    for r0 in range(0, n, b):
        q0 = r0 // 8
        N = M[q0 : q0 + H]

        def column(k):
            return [
                jnp.broadcast_to(N[h][:, r0 + k : r0 + k + 1], (8, n)) if h >= k // 8 else None for h in range(H)]

        S = {k: column(k) for k in range(ahead[0])}
        have = ahead[0]
        scale = [None] * H
        d = spread(S[0][0], 0)
        for j in range(b):
            hj, sj = j // 8, j % 8
            rs = lax.rsqrt(d)
            scale[hj] = rs if sj == 0 else jnp.where(sub == sj, rs, scale[hj])
            here = lane == r0 + j
            N[hj] = jnp.where(here, jnp.where(sub == sj, 1.0, 0.0), N[hj])
            if j == b - 1:
                break
            C = S.pop(j)
            row = {k: spread(C[k // 8], k % 8) for k in S}
            rinv = rs * rs
            hn, sn = (j + 1) // 8, (j + 1) % 8
            d = spread(S[j + 1][hn], sn) - (row[j + 1] * row[j + 1]) * rinv
            u = [C[h] * rinv if h >= hj else None for h in range(H)]
            for k in S:
                S[k] = [S[k][h] - u[h] * row[k] if h >= k // 8 else None for h in range(H)]
            prow = spread(N[hj], sj)
            for h in range(hj, H):
                if h > hj:
                    N[h] = jnp.where(here, 0.0, N[h]) - u[h] * prow
                elif sj < 7:
                    N[h] = N[h] - jnp.where(sub > sj, u[h], 0.0) * prow
            while have < min(b, j + 1 + ahead[3 * j // b]):
                S[have] = column(have)
                have += 1
        N = [N[h] * scale[h] for h in range(H)]
        for h in range(H):
            M[q0 + h] = jnp.where(lane <= sub + (r0 + 8 * h), N[h], 0.0)
        if r0 + b < n:
            X = [
                jnp.where((lane > sub + (r0 + 8 * h)) & (lane < r0 + b), 0.0, N[h]) for h in range(H)]
            h_, m_, l_ = split3(jnp.concatenate(X, axis=0))
            R = tn(jnp.concatenate([h_, h_, m_, h_, l_, m_], 0), jnp.concatenate([h_, m_, h_, l_, h_, m_], 0))
            inblk = (lane >= r0) & (lane < r0 + b)
            for q in range(q0 + H, n // 8):
                M[q] = jnp.where(inblk, 0.0, M[q]) - R[8 * q : 8 * q + 8, :]
    return jnp.concatenate(M, axis=0)


def kernel(a_ref, yr, yc, damp_ref, akk, bc, br, zb, tz, tx, dn, wst, lh, ll, kh, kl, g0, g1, ph, pm,
           w_ref, zs, zr, zd, vs, vr, ts, tr, xs, xr, ks, kr, kd, hs, hr, us, ur, ds, dr):
    i = lax.axis_index("row")
    j = lax.axis_index("col")
    z = j // 2
    c = lax.rem(j, 2)
    partner = (i, 2 * z + 1 - c)

    def zpeer(d):
        return (i, 2 * lax.rem(z + d, 16) + c)

    def xpeer(d):
        return (lax.rem(i + d, 16), j)

    def copy(src, dst, ssem, rsem, dev):
        return pltpu.make_async_remote_copy(
            src_ref=src, dst_ref=dst, send_sem=ssem, recv_sem=rsem, device_id=dev, device_id_type=MESH)

    def each(lo, hi, f):
        def step(d, carry):
            f(d)
            return carry
        lax.fori_loop(lo, hi, step, 0)

    barrier = pltpu.get_barrier_semaphore()

    def greet(d):
        pl.semaphore_signal(barrier, inc=1, device_id=zpeer(d), device_id_type=MESH)
        pl.semaphore_signal(barrier, inc=1, device_id=xpeer(d), device_id_type=MESH)

    each(1, 16, greet)
    pl.semaphore_signal(barrier, inc=1, device_id=partner, device_id_type=MESH)

    lane = lax.broadcasted_iota(jnp.int32, (32, 128), 1)
    V = jnp.concatenate([a_ref[0:32, 0:128], a_ref[256:288, 0:128], jnp.zeros((64, 128), F32)], 0).T[0:32, :]
    v0 = jnp.where(lane < 16, V, pltpu.roll(V, 112, 1))
    v1 = jnp.where(lane < 16, pltpu.roll(V, 112, 1), pltpu.roll(V, 96, 1))
    part = lane[0:8, :]
    zb[0, z, c] = jnp.where(
        part < 32, v0[0:8, :],
        jnp.where(part < 64, pltpu.roll(v0[8:16, :], 32, 1),
                  jnp.where(part < 96, pltpu.roll(v0[16:24, :], 64, 1), pltpu.roll(v0[24:32, :], 96, 1))))
    zb[1, z, c] = jnp.where(part < 32, v1[16:24, :], pltpu.roll(v1[24:32, :], 32, 1))
    r = lax.broadcasted_iota(jnp.int32, (256, 256), 0)
    q = lax.broadcasted_iota(jnp.int32, (256, 256), 1)
    own = a_ref[pl.ds(pl.multiple_of(256 * c, 256), 256), :]
    t = jnp.sum(jnp.where((r == q) & (z == i), own, 0.0), axis=0, keepdims=True)
    tz[z, c] = jnp.broadcast_to(jnp.sum(t, axis=1, keepdims=True), (1, 128))

    pl.semaphore_wait(barrier, 31)

    def behind(v, d):
        return lax.rem(v + 16 - d, 16)

    def z_copy(d, s):
        return copy(zb.at[0, s, c], zb.at[0, s, c], zs.at[d], zr.at[d], zpeer(d))

    def v_copy(d, s):
        return copy(zb.at[1, s, c], zb.at[1, s, c], vs.at[d], vr.at[d], zpeer(d))

    def t_copy(d, s):
        return copy(tz.at[s, c], tz.at[s, c], ts.at[d], tr.at[d], zpeer(d))

    def x_copy(d, s):
        return copy(bc.at[:, s], bc.at[:, s], xs.at[d], xr.at[d], xpeer(d))

    def h_copy(d, s):
        return copy(tx.at[s], tx.at[s], hs.at[d], hr.at[d], xpeer(d))

    def lanes(n, x):
        return pl.ds(512, 512) if n == 1 else pl.ds((512 if n else 0) + NB * x, 512 - NB * x)

    def k_send(n, x, d):
        v = akk.at[n // 2, i, c, :, lanes(n, x)]
        return copy(v, v, ks.at[n, d], kr.at[n, i], xpeer(d))

    def k_sends(n, f):
        for x in range(1 if n == 1 else 4):
            if n == 1:
                each(1, 16, lambda d: f(k_send(n, x, d)))
            else:

                @pl.when(i // 4 == x)
                def _():
                    each(1, 16, lambda d: f(k_send(n, x, d)))

    def k_recv(n, xs=(0, 1, 2, 3)):
        for x in xs:

            def one(s, carry):
                @pl.when(s != i)
                def _():
                    v = akk.at[n // 2, s, c, :, lanes(n, x)]
                    copy(v, v, ks.at[n, 0], kr.at[n, s], partner).wait_recv()
                return carry

            lax.fori_loop(4 * x, 4 * x + 4, one, 0)

    def k_pair(n, x, h):
        v = akk.at[n // 2, pl.ds(4 * x, 4), h, :, lanes(n, x)]
        return copy(v, v, kd.at[0, n, x], kd.at[1, n, x], partner)

    def k_pairs(n, h, f):
        for x in range(4):
            f(k_pair(n, x, h))

    def begin(v):
        v.start()

    def arrived(v):
        v.wait_recv()

    def left(v):
        v.wait_send()

    def z_pair(h):
        return copy(zb.at[0, :, h], zb.at[0, :, h], zd.at[0], zd.at[1], partner)

    def v_pair(h):
        return copy(zb.at[1, :, h], zb.at[1, :, h], zd.at[4], zd.at[5], partner)

    def t_pair(h):
        return copy(tz.at[:, h], tz.at[:, h], zd.at[2], zd.at[3], partner)

    up_to = (i, 2 * lax.rem(z + 1, 16) + c)
    down_to = (i, 2 * lax.rem(z + 15, 16) + c)

    def ring(s, up, arriving=False):
        e = s + 1 if arriving else s
        k = behind(z, e) if up else lax.rem(z + e, 16)
        o = 0 if up else 8
        return [
            copy(br.at[p, k, c], br.at[p, k, c], us.at[p, s + o], ur.at[p, s + o], up_to if up else down_to)
            for p in range(2)]

    def pair(k, h):
        return copy(br.at[:, k, h], br.at[:, k, h], ds.at[k], dr.at[k], partner)

    def ring_step(s):
        for p in range(2):
            ring(s - 1, True, True)[p].wait_recv()
            ring(s, True)[p].start()
            ring(s - 1, False, True)[p].wait_recv()
            if s < 7:
                ring(s, False)[p].start()
        pair(behind(z, s), c).start()
        pair(lax.rem(z + s, 16), c).start()

    def ring_end():
        for p in range(2):
            ring(7, True, True)[p].wait_recv()
        pair(lax.rem(z + 8, 16), c).start()

    def assembled(n):
        p = zb[n].reshape(32, 1, 8, 128)
        two = pltpu.roll(p.reshape(256, 128), 96, 1).reshape(32, 1, 8, 128)
        return jnp.concatenate([p, two], axis=1).reshape(512, 128).T

    each(1, 16, lambda d: z_copy(d, z).start())
    each(1, 16, lambda d: t_copy(d, z).start())
    T = a_ref[:, 0:128].T
    br[0, z, c] = T[0:16, :]
    br[1, z, c] = T[16:32, :]
    for p in range(2):
        for h in range(2):
            bc[p, i, h] = a_ref[256 * h + 16 * p : 256 * h + 16 * p + 16, :]
    for p in range(2):
        ring(0, True)[p].start()
        ring(0, False)[p].start()
    each(1, 16, lambda d: v_copy(d, z).start())
    pair(z, c).start()
    each(1, 16, lambda d: x_copy(d, i).start())
    each(1, 16, lambda d: z_copy(d, behind(z, d)).wait_recv())
    z_pair(c).start()
    each(1, 16, lambda d: t_copy(d, behind(z, d)).wait_recv())
    t_pair(c).start()
    ring_step(1)
    z_pair(1 - c).wait_recv()
    S = assembled(0)
    akk[0, i, c, :, 0:512] = jnp.where(c == 0, S[0:16, :], S[16:32, :])
    t_pair(1 - c).wait_recv()
    tx[i] = jnp.sum(tz[...].reshape(32, 1, 128), axis=0)
    each(1, 16, lambda d: h_copy(d, i).start())
    k_sends(0, begin)
    ring_step(2)
    akk[0, i, c, :, 512:1024] = jnp.where(c == 0, S[64:80, :], S[80:96, :])
    each(1, 16, lambda d: v_copy(d, behind(z, d)).wait_recv())
    v_pair(c).start()
    v_pair(1 - c).wait_recv()
    ring_step(3)
    S = assembled(1)
    akk[1, i, c, :, 512:1024] = jnp.where(c == 0, S[0:16, :], S[16:32, :])
    each(1, 16, lambda d: h_copy(d, behind(i, d)).wait_recv())
    damp = jnp.sum(tx[...], axis=0) * (damping_share / 8192.0)
    damp_ref[...] = jnp.broadcast_to(damp, (8, 128))
    k_recv(0, (0,))
    k_pair(0, 0, c).start()
    k_recv(0, (1, 2, 3))
    for x in (1, 2, 3):
        k_pair(0, x, c).start()
    k_sends(1, begin)
    k_sends(2, begin)
    ring_step(4)
    k_pair(0, 0, 1 - c).wait_recv()

    damp2 = jnp.concatenate([damp, damp], axis=1)
    damp4 = jnp.concatenate([damp2, damp2], axis=1)
    eye = lax.broadcasted_iota(jnp.int32, (NB, NB), 0) == lax.broadcasted_iota(jnp.int32, (NB, NB), 1)
    deye = jnp.where(eye, damp, 0.0)
    ln = lax.broadcasted_iota(jnp.int32, (PS, 512), 1)
    posl = jnp.where(ln % 256 < 32, (ln % 256 // 16) * 512 + (2 * i + ln // 256) * 16 + ln % 16, -1)
    posr = lax.broadcasted_iota(jnp.int32, (PS, 512), 0)

    dn[...] = akk[0, 0:4, :, :, 0:NB].reshape(NB, NB)

    def middle():
        ring_end()
        each(1, 16, lambda d: x_copy(d, behind(i, d)).wait_recv())
        k_pairs(1, 1 - c, arrived)
        k_pairs(2, 1 - c, arrived)
        each(0, 16, lambda k: pair(k, 1 - c).wait_recv())
        for b in range(4):
            o = b * NB
            rows = slice(o, o + NB)
            acc = jnp.concatenate([
                akk[0, 4 * b : 4 * b + 4, :, :, 512:1024].reshape(NB, 512),
                bc[0, 4 * b : 4 * b + 4].reshape(NB, 256),
                br[0, 4 * b : 4 * b + 4].reshape(NB, 512) + jnp.where(posr[rows] == posl[rows], damp4, 0.0)], axis=1)
            if b:
                acc = acc - nn(
                    jnp.concatenate([lh[rows, 0:o], ll[rows, 0:o], lh[rows, 0:o]], axis=1),
                    jnp.concatenate([ph[0:o, :], ph[0:o, :], pm[0:o, :]], axis=0))
            Y = nn(wst[b], right3(*split2(acc)))
            yr[rows, :] = Y[:, PS + 256 :]
            yc[rows, :] = Y[:, PS : PS + 256]
            ph[rows, :], pm[rows, :] = split2(Y)
            th, tl = split2(Y[:, 0:PS].T)
            kh[:, o : o + NB] = th
            kl[:, o : o + NB] = tl
        lhs = jnp.concatenate([kh[...], kl[...], kh[...]], axis=1)
        for o in range(0, RW, 256):
            R = nn(lhs, jnp.concatenate([ph[:, o : o + 256], ph[:, o : o + 256], pm[:, o : o + 256]], axis=0))
            if o < PS:
                src = akk[1, :, :, :, 512 + o : 768 + o].reshape(512, 256)
            elif o == PS:
                src = bc[1].reshape(512, 256)
            else:
                v = o - PS - 256
                src = br[1, :, :, :, v : v + 256].reshape(512, 256) + jnp.where(
                    posr[:, v : v + 256] + 512 == posl[:, v : v + 256], damp2, 0.0)
            g1[:, o : o + 256] = src - R
        dn[...] = g1[0:NB, 0:NB]

    def body(b, carry):
        w_ref[...] = block_inverse(dn[...] + deye)
        for k in range(8):

            @pl.when(b == k)
            def _():
                wl = left3(*split2(w_ref[...]))
                kk = k % 4
                lo = (kk + 1) * NB
                rows = slice(kk * NB, lo)
                if k < 4:
                    wst[k] = wl
                    if k < 3:
                        ring_step(5 + k)
                    if k == 0:
                        for x in (1, 2, 3):
                            k_pair(0, x, 1 - c).wait_recv()
                        g0[...] = akk[0, :, :, :, 0:512].reshape(512, 512)
                    if k == 2:
                        k_recv(1)
                        k_pairs(1, c, begin)
                        k_recv(2)
                        k_pairs(2, c, begin)
                    if k == 3:
                        middle()
                        return
                    g, hi = g0, PS
                else:
                    g, hi = g1, RW
                Y = nn(wl, right3(*split2(g[rows, lo:hi])))
                h, l = split2(Y)
                if k >= 4:
                    yr[PS + kk * NB : PS + lo, :] = Y[:, PS + 256 - lo :]
                    yc[PS + kk * NB : PS + lo, :] = Y[:, PS - lo : PS + 256 - lo]
                if kk < 3:
                    th, tl = split2(Y[:, 0 : PS - lo].T)
                    if k < 4:
                        lh[lo:PS, rows] = th
                        ll[lo:PS, rows] = tl
                    lhs = left3(th, tl)
                    right = right3(h, l)
                    for o in range(0, hi - lo, 256):
                        e = min(o + 256, hi - lo)
                        g[lo:PS, lo + o : lo + e] = g[lo:PS, lo + o : lo + e] - nn(lhs, right[:, o:e])
                    dn[...] = g[lo : lo + NB, lo : lo + NB]
        return carry

    lax.fori_loop(0, 8, body, 0)

    each(1, 16, lambda d: z_copy(d, z).wait_send())
    each(1, 16, lambda d: v_copy(d, z).wait_send())
    v_pair(c).wait_send()
    each(1, 16, lambda d: t_copy(d, z).wait_send())
    each(1, 16, lambda d: x_copy(d, i).wait_send())
    each(1, 16, lambda d: h_copy(d, i).wait_send())
    for n in range(3):
        k_sends(n, left)
        k_pairs(n, c, left)
    for s in range(8):
        for p in range(2):
            ring(s, True)[p].wait_send()
            if s < 7:
                ring(s, False)[p].wait_send()
    each(0, 16, lambda k: pair(k, c).wait_send())
    z_pair(c).wait_send()
    t_pair(c).wait_send()


def finish(a_ref, yr, yc, damp_ref, out_ref):
    i = lax.axis_index("row")
    j = lax.axis_index("col")
    r = lax.broadcasted_iota(jnp.int32, (512, 256), 0)
    q = lax.broadcasted_iota(jnp.int32, (512, 256), 1)
    U = jnp.zeros((512, 256), F32)
    for o in (0, PS):
        th, tl = split2(yr[o : o + PS, :].T)
        U = U + nn(left3(th, tl), right3(*split2(yc[o : o + PS, :])))
    at = [pl.ds(pl.multiple_of(j * 16 + o, 16), 16) for o in (0, PS)]
    cols = jnp.concatenate([yr[at[0], :], yr[at[1], :], jnp.zeros((96, 512), F32)], 0).T
    rm = r % 256
    posrow = jnp.where(rm < 32, (rm // 16) * 512 + (2 * i + r // 256) * 16 + rm % 16, 1024)
    poscol = (q // 16) * 512 + j * 16 + q % 16
    damp = damp_ref[0:1, :]
    damp2 = jnp.concatenate([damp, damp], axis=1)
    A = a_ref[...] + jnp.where(r + 512 * i == q + 256 * j, damp2, 0.0)
    cols = jnp.concatenate([cols, jnp.zeros((512, 128), F32)], 1)
    out_ref[...] = jnp.where(
        q >= 32, jnp.where(rm >= 32, A - U, 0.0), jnp.where(posrow >= poscol, cols, 0.0))


def on_device(factors):
    vm = pl.BlockSpec(memory_space=pltpu.VMEM)
    dma = pltpu.SemaphoreType.DMA
    v = pltpu.VMEM
    f = jax.ShapeDtypeStruct
    parts = pl.pallas_call(
        kernel,
        out_shape=[f((1024, 512), F32), f((1024, 256), F32), f((8, 128), F32)],
        in_specs=[vm],
        out_specs=[vm] * 3,
        scratch_shapes=[
            v((2, 16, 2, 16, 1024), F32), v((2, 16, 2, 16, 256), F32),
            v((2, 16, 2, 16, 512), F32), v((2, 16, 2, 8, 128), F32), v((16, 2, 1, 128), F32), v((16, 1, 128), F32),
            v((NB, NB), F32), v((4, NB, 3 * NB), BF16), v((PS, PS), BF16), v((PS, PS), BF16), v((PS, PS), BF16),
            v((PS, PS), BF16), v((PS, PS), F32), v((PS, RW), F32), v((PS, RW), BF16), v((PS, RW), BF16),
            v((NB, NB), F32),
            dma((16,)), dma((16,)), dma((6,)), dma((16,)), dma((16,)), dma((16,)), dma((16,)), dma((16,)), dma((16,)),
            dma((3, 16)), dma((3, 16)), dma((2, 3, 4)), dma((16,)), dma((16,)), dma((2, 16)), dma((2, 16)),
            dma((16,)), dma((16,)),
        ],
        compiler_params=pltpu.CompilerParams(
            collective_id=0, has_side_effects=True, vmem_limit_bytes=42 * 1024 * 1024),
        name="gather_eliminate",
    )(factors[0])
    out = pl.pallas_call(
        finish,
        out_shape=f((512, 256), F32),
        in_specs=[vm] * 4,
        out_specs=vm,
        compiler_params=pltpu.CompilerParams(vmem_limit_bytes=16 * 1024 * 1024),
        name="finish",
    )(factors[0], *parts)
    return out[None]


def solution(mesh):
    placed = P(None, "row", "col")
    return jax.shard_map(on_device, mesh=mesh, in_specs=(placed,), out_specs=placed, check_vma=False)
```

```python
import jax
import jax.numpy as jnp
from jax import lax
from jax.experimental import pallas as pl
from jax.experimental.pallas import tpu as pltpu
from jax.sharding import PartitionSpec as P

F32, BF16 = jnp.float32, jnp.bfloat16
MESH = pl.DeviceIdType.MESH
damping_share = 0.03162277660168379
NB = 128
MINI = 64
AHEAD = (6, 6, 7)
PS = 512
RW = PS + 256 + 512


def split3(x):
    h = x.astype(BF16)
    r = x - h.astype(F32)
    m = r.astype(BF16)
    return h, m, (r - m.astype(F32)).astype(BF16)


def split2(x):
    h = x.astype(BF16)
    return h, (x - h.astype(F32)).astype(BF16)


def tn(a, b):
    return lax.dot_general(a, b, (((0,), (0,)), ((), ())), preferred_element_type=F32)


def nn(a, b):
    return lax.dot_general(a, b, (((1,), (0,)), ((), ())), preferred_element_type=F32)


def left3(h, l):
    return jnp.concatenate([h, l, h], axis=1)


def right3(h, l):
    return jnp.concatenate([h, h, l], axis=0)


def block_inverse(M, b=MINI, ahead=AHEAD):
    n = NB
    H = b // 8
    sub = lax.broadcasted_iota(jnp.int32, (8, n), 0)
    lane = lax.broadcasted_iota(jnp.int32, (8, n), 1)

    def spread(x, s):
        return jnp.broadcast_to(x[s : s + 1, :], (8, n))

    M = [M[8 * q : 8 * q + 8, :] for q in range(n // 8)]
    for r0 in range(0, n, b):
        q0 = r0 // 8
        N = M[q0 : q0 + H]

        def column(k):
            return [
                jnp.broadcast_to(N[h][:, r0 + k : r0 + k + 1], (8, n)) if h >= k // 8 else None for h in range(H)]

        S = {k: column(k) for k in range(ahead[0])}
        have = ahead[0]
        scale = [None] * H
        d = spread(S[0][0], 0)
        for j in range(b):
            hj, sj = j // 8, j % 8
            rs = lax.rsqrt(d)
            scale[hj] = rs if sj == 0 else jnp.where(sub == sj, rs, scale[hj])
            here = lane == r0 + j
            N[hj] = jnp.where(here, jnp.where(sub == sj, 1.0, 0.0), N[hj])
            if j == b - 1:
                break
            C = S.pop(j)
            row = {k: spread(C[k // 8], k % 8) for k in S}
            rinv = rs * rs
            hn, sn = (j + 1) // 8, (j + 1) % 8
            d = spread(S[j + 1][hn], sn) - (row[j + 1] * row[j + 1]) * rinv
            u = [C[h] * rinv if h >= hj else None for h in range(H)]
            for k in S:
                S[k] = [S[k][h] - u[h] * row[k] if h >= k // 8 else None for h in range(H)]
            prow = spread(N[hj], sj)
            for h in range(hj, H):
                if h > hj:
                    N[h] = jnp.where(here, 0.0, N[h]) - u[h] * prow
                elif sj < 7:
                    N[h] = N[h] - jnp.where(sub > sj, u[h], 0.0) * prow
            while have < min(b, j + 1 + ahead[3 * j // b]):
                S[have] = column(have)
                have += 1
        N = [N[h] * scale[h] for h in range(H)]
        for h in range(H):
            M[q0 + h] = jnp.where(lane <= sub + (r0 + 8 * h), N[h], 0.0)
        if r0 + b < n:
            X = [
                jnp.where((lane > sub + (r0 + 8 * h)) & (lane < r0 + b), 0.0, N[h]) for h in range(H)]
            h_, m_, l_ = split3(jnp.concatenate(X, axis=0))
            R = tn(jnp.concatenate([h_, h_, m_, h_, l_, m_], 0), jnp.concatenate([h_, m_, h_, l_, h_, m_], 0))
            inblk = (lane >= r0) & (lane < r0 + b)
            for q in range(q0 + H, n // 8):
                M[q] = jnp.where(inblk, 0.0, M[q]) - R[8 * q : 8 * q + 8, :]
    return jnp.concatenate(M, axis=0)


def kernel(a_ref, yr, yc, damp_ref, akk, bc, br, zb, tz, tx, dn, wst, lh, ll, kh, kl, g0, g1, ph, pm,
           w_ref, zs, zr, zd, vs, vr, ts, tr, xs, xr, ks, kr, kd, hs, hr, us, ur, ds, dr):
    i = lax.axis_index("row")
    j = lax.axis_index("col")
    z = j // 2
    c = lax.rem(j, 2)
    partner = (i, 2 * z + 1 - c)

    def zpeer(d):
        return (i, 2 * lax.rem(z + d, 16) + c)

    def xpeer(d):
        return (4 * lax.rem(i // 4 + d // 4, 4) + lax.rem(i + d, 4), j)

    def xfrom(d):
        return 4 * lax.rem(i // 4 + 4 - d // 4, 4) + lax.rem(i + 4 - lax.rem(d, 4), 4)

    def copy(src, dst, ssem, rsem, dev):
        return pltpu.make_async_remote_copy(
            src_ref=src, dst_ref=dst, send_sem=ssem, recv_sem=rsem, device_id=dev, device_id_type=MESH)

    def each(lo, hi, f):
        def step(d, carry):
            f(d)
            return carry
        lax.fori_loop(lo, hi, step, 0)

    barrier = pltpu.get_barrier_semaphore()

    def greet(d):
        pl.semaphore_signal(barrier, inc=1, device_id=zpeer(d), device_id_type=MESH)
        pl.semaphore_signal(barrier, inc=1, device_id=xpeer(d), device_id_type=MESH)

    each(1, 16, greet)
    pl.semaphore_signal(barrier, inc=1, device_id=partner, device_id_type=MESH)

    lane = lax.broadcasted_iota(jnp.int32, (32, 128), 1)
    V = jnp.concatenate([a_ref[0:32, 0:128], a_ref[256:288, 0:128], jnp.zeros((64, 128), F32)], 0).T[0:32, :]
    v0 = jnp.where(lane < 16, V, pltpu.roll(V, 112, 1))
    v1 = jnp.where(lane < 16, pltpu.roll(V, 112, 1), pltpu.roll(V, 96, 1))
    part = lane[0:8, :]
    zb[0, z, c] = jnp.where(
        part < 32, v0[0:8, :],
        jnp.where(part < 64, pltpu.roll(v0[8:16, :], 32, 1),
                  jnp.where(part < 96, pltpu.roll(v0[16:24, :], 64, 1), pltpu.roll(v0[24:32, :], 96, 1))))
    zb[1, z, c] = jnp.where(part < 32, v1[16:24, :], pltpu.roll(v1[24:32, :], 32, 1))
    r = lax.broadcasted_iota(jnp.int32, (256, 256), 0)
    q = lax.broadcasted_iota(jnp.int32, (256, 256), 1)
    own = a_ref[pl.ds(pl.multiple_of(256 * c, 256), 256), :]
    t = jnp.sum(jnp.where((r == q) & (z == i), own, 0.0), axis=0, keepdims=True)
    tz[z, c] = jnp.broadcast_to(jnp.sum(t, axis=1, keepdims=True), (1, 128))

    pl.semaphore_wait(barrier, 31)

    def behind(v, d):
        return lax.rem(v + 16 - d, 16)

    def z_copy(d, s):
        return copy(zb.at[0, s, c], zb.at[0, s, c], zs.at[d], zr.at[d], zpeer(d))

    def v_copy(d, s):
        return copy(zb.at[1, s, c], zb.at[1, s, c], vs.at[d], vr.at[d], zpeer(d))

    def t_copy(d, s):
        return copy(tz.at[s, c], tz.at[s, c], ts.at[d], tr.at[d], zpeer(d))

    def x_copy(d, s):
        return copy(bc.at[:, s], bc.at[:, s], xs.at[d], xr.at[d], xpeer(d))

    def h_copy(d, s):
        return copy(tx.at[s], tx.at[s], hs.at[d], hr.at[d], xpeer(d))

    def lanes(n, x):
        return pl.ds(512, 512) if n == 1 else pl.ds((512 if n else 0) + NB * x, 512 - NB * x)

    def k_send(n, x, d):
        v = akk.at[n // 2, i, c, :, lanes(n, x)]
        return copy(v, v, ks.at[n, d], kr.at[n, i], xpeer(d))

    def k_sends(n, f):
        for x in range(1 if n == 1 else 4):
            if n == 1:
                each(1, 16, lambda d: f(k_send(n, x, d)))
            else:

                @pl.when(i // 4 == x)
                def _():
                    each(1, 16, lambda d: f(k_send(n, x, d)))

    def k_recv(n, xs=(0, 1, 2, 3)):
        for x in xs:

            def one(s, carry):
                @pl.when(s != i)
                def _():
                    v = akk.at[n // 2, s, c, :, lanes(n, x)]
                    copy(v, v, ks.at[n, 0], kr.at[n, s], partner).wait_recv()
                return carry

            lax.fori_loop(4 * x, 4 * x + 4, one, 0)

    def k_pair(n, x, h):
        v = akk.at[n // 2, pl.ds(4 * x, 4), h, :, lanes(n, x)]
        return copy(v, v, kd.at[0, n, x], kd.at[1, n, x], partner)

    def k_pairs(n, h, f):
        for x in range(4):
            f(k_pair(n, x, h))

    def begin(v):
        v.start()

    def arrived(v):
        v.wait_recv()

    def left(v):
        v.wait_send()

    def z_pair(h):
        return copy(zb.at[0, :, h], zb.at[0, :, h], zd.at[0], zd.at[1], partner)

    def v_pair(h):
        return copy(zb.at[1, :, h], zb.at[1, :, h], zd.at[4], zd.at[5], partner)

    def t_pair(h):
        return copy(tz.at[:, h], tz.at[:, h], zd.at[2], zd.at[3], partner)

    up_to = (i, 2 * lax.rem(z + 1, 16) + c)
    down_to = (i, 2 * lax.rem(z + 15, 16) + c)

    def ring(s, up, arriving=False):
        e = s + 1 if arriving else s
        k = behind(z, e) if up else lax.rem(z + e, 16)
        o = 0 if up else 8
        return [
            copy(br.at[p, k, c], br.at[p, k, c], us.at[p, s + o], ur.at[p, s + o], up_to if up else down_to)
            for p in range(2)]

    def pair(k, h):
        return copy(br.at[:, k, h], br.at[:, k, h], ds.at[k], dr.at[k], partner)

    def ring_step(s):
        for p in range(2):
            ring(s - 1, True, True)[p].wait_recv()
            ring(s, True)[p].start()
            ring(s - 1, False, True)[p].wait_recv()
            if s < 7:
                ring(s, False)[p].start()
        pair(behind(z, s), c).start()
        pair(lax.rem(z + s, 16), c).start()

    def ring_end():
        for p in range(2):
            ring(7, True, True)[p].wait_recv()
        pair(lax.rem(z + 8, 16), c).start()

    def assembled(n):
        p = zb[n].reshape(32, 1, 8, 128)
        two = pltpu.roll(p.reshape(256, 128), 96, 1).reshape(32, 1, 8, 128)
        return jnp.concatenate([p, two], axis=1).reshape(512, 128).T

    each(1, 16, lambda d: z_copy(d, z).start())
    each(1, 16, lambda d: t_copy(d, z).start())
    T = a_ref[:, 0:128].T
    br[0, z, c] = T[0:16, :]
    br[1, z, c] = T[16:32, :]
    for p in range(2):
        for h in range(2):
            bc[p, i, h] = a_ref[256 * h + 16 * p : 256 * h + 16 * p + 16, :]
    for p in range(2):
        ring(0, True)[p].start()
        ring(0, False)[p].start()
    each(1, 16, lambda d: v_copy(d, z).start())
    pair(z, c).start()
    each(1, 16, lambda d: x_copy(d, i).start())
    each(1, 16, lambda d: z_copy(d, behind(z, d)).wait_recv())
    z_pair(c).start()
    each(1, 16, lambda d: t_copy(d, behind(z, d)).wait_recv())
    t_pair(c).start()
    ring_step(1)
    z_pair(1 - c).wait_recv()
    S = assembled(0)
    akk[0, i, c, :, 0:512] = jnp.where(c == 0, S[0:16, :], S[16:32, :])
    t_pair(1 - c).wait_recv()
    tx[i] = jnp.sum(tz[...].reshape(32, 1, 128), axis=0)
    each(1, 16, lambda d: h_copy(d, i).start())
    k_sends(0, begin)
    ring_step(2)
    akk[0, i, c, :, 512:1024] = jnp.where(c == 0, S[64:80, :], S[80:96, :])
    each(1, 16, lambda d: v_copy(d, behind(z, d)).wait_recv())
    v_pair(c).start()
    v_pair(1 - c).wait_recv()
    ring_step(3)
    S = assembled(1)
    akk[1, i, c, :, 512:1024] = jnp.where(c == 0, S[0:16, :], S[16:32, :])
    each(1, 16, lambda d: h_copy(d, xfrom(d)).wait_recv())
    damp = jnp.sum(tx[...], axis=0) * (damping_share / 8192.0)
    damp_ref[...] = jnp.broadcast_to(damp, (8, 128))
    k_recv(0, (0,))
    k_pair(0, 0, c).start()
    k_sends(1, begin)
    k_sends(2, begin)
    k_recv(0, (1, 2, 3))
    for x in (1, 2, 3):
        k_pair(0, x, c).start()
    ring_step(4)
    k_pair(0, 0, 1 - c).wait_recv()

    damp2 = jnp.concatenate([damp, damp], axis=1)
    damp4 = jnp.concatenate([damp2, damp2], axis=1)
    eye = lax.broadcasted_iota(jnp.int32, (NB, NB), 0) == lax.broadcasted_iota(jnp.int32, (NB, NB), 1)
    deye = jnp.where(eye, damp, 0.0)
    ln = lax.broadcasted_iota(jnp.int32, (PS, 512), 1)
    posl = jnp.where(ln % 256 < 32, (ln % 256 // 16) * 512 + (2 * i + ln // 256) * 16 + ln % 16, -1)
    posr = lax.broadcasted_iota(jnp.int32, (PS, 512), 0)

    dn[...] = akk[0, 0:4, :, :, 0:NB].reshape(NB, NB)

    def middle():
        each(1, 16, lambda d: x_copy(d, xfrom(d)).wait_recv())
        k_pairs(1, 1 - c, arrived)
        k_pairs(2, 1 - c, arrived)
        each(0, 16, lambda k: pair(k, 1 - c).wait_recv())
        for b in range(4):
            o = b * NB
            rows = slice(o, o + NB)
            acc = jnp.concatenate([
                akk[0, 4 * b : 4 * b + 4, :, :, 512:1024].reshape(NB, 512),
                bc[0, 4 * b : 4 * b + 4].reshape(NB, 256),
                br[0, 4 * b : 4 * b + 4].reshape(NB, 512) + jnp.where(posr[rows] == posl[rows], damp4, 0.0)], axis=1)
            if b:
                acc = acc - nn(
                    jnp.concatenate([lh[rows, 0:o], ll[rows, 0:o], lh[rows, 0:o]], axis=1),
                    jnp.concatenate([ph[0:o, :], ph[0:o, :], pm[0:o, :]], axis=0))
            Y = nn(wst[b], right3(*split2(acc)))
            yr[rows, :] = Y[:, PS + 256 :]
            yc[rows, :] = Y[:, PS : PS + 256]
            ph[rows, :], pm[rows, :] = split2(Y)
            th, tl = split2(Y[:, 0:PS].T)
            kh[:, o : o + NB] = th
            kl[:, o : o + NB] = tl
        lhs = jnp.concatenate([kh[...], kl[...], kh[...]], axis=1)
        for o in range(0, RW, 256):
            R = nn(lhs, jnp.concatenate([ph[:, o : o + 256], ph[:, o : o + 256], pm[:, o : o + 256]], axis=0))
            if o < PS:
                src = akk[1, :, :, :, 512 + o : 768 + o].reshape(512, 256)
            elif o == PS:
                src = bc[1].reshape(512, 256)
            else:
                v = o - PS - 256
                src = br[1, :, :, :, v : v + 256].reshape(512, 256) + jnp.where(
                    posr[:, v : v + 256] + 512 == posl[:, v : v + 256], damp2, 0.0)
            g1[:, o : o + 256] = src - R
        dn[...] = g1[0:NB, 0:NB]

    def body(b, carry):
        w_ref[...] = block_inverse(dn[...] + deye)
        for k in range(8):

            @pl.when(b == k)
            def _():
                wl = left3(*split2(w_ref[...]))
                kk = k % 4
                lo = (kk + 1) * NB
                rows = slice(kk * NB, lo)
                if k < 4:
                    wst[k] = wl
                    if k < 3:
                        ring_step(5 + k)
                    if k == 0:
                        for x in (1, 2, 3):
                            k_pair(0, x, 1 - c).wait_recv()
                        g0[...] = akk[0, :, :, :, 0:512].reshape(512, 512)
                    if k == 2:
                        k_recv(1)
                        k_pairs(1, c, begin)
                        k_recv(2)
                        k_pairs(2, c, begin)
                        ring_end()
                    if k == 3:
                        middle()
                        return
                    g, hi = g0, PS
                else:
                    g, hi = g1, RW
                Y = nn(wl, right3(*split2(g[rows, lo:hi])))
                h, l = split2(Y)
                if k >= 4:
                    yr[PS + kk * NB : PS + lo, :] = Y[:, PS + 256 - lo :]
                    yc[PS + kk * NB : PS + lo, :] = Y[:, PS - lo : PS + 256 - lo]
                if kk < 3:
                    th, tl = split2(Y[:, 0 : PS - lo].T)
                    if k < 4:
                        lh[lo:PS, rows] = th
                        ll[lo:PS, rows] = tl
                    lhs = left3(th, tl)
                    right = right3(h, l)
                    for o in range(0, hi - lo, 256):
                        e = min(o + 256, hi - lo)
                        g[lo:PS, lo + o : lo + e] = g[lo:PS, lo + o : lo + e] - nn(lhs, right[:, o:e])
                    dn[...] = g[lo : lo + NB, lo : lo + NB]
        return carry

    lax.fori_loop(0, 8, body, 0)

    each(1, 16, lambda d: z_copy(d, z).wait_send())
    each(1, 16, lambda d: v_copy(d, z).wait_send())
    v_pair(c).wait_send()
    each(1, 16, lambda d: t_copy(d, z).wait_send())
    each(1, 16, lambda d: x_copy(d, i).wait_send())
    each(1, 16, lambda d: h_copy(d, i).wait_send())
    for n in range(3):
        k_sends(n, left)
        k_pairs(n, c, left)
    for s in range(8):
        for p in range(2):
            ring(s, True)[p].wait_send()
            if s < 7:
                ring(s, False)[p].wait_send()
    each(0, 16, lambda k: pair(k, c).wait_send())
    z_pair(c).wait_send()
    t_pair(c).wait_send()


def finish(a_ref, yr, yc, damp_ref, out_ref):
    i = lax.axis_index("row")
    j = lax.axis_index("col")
    r = lax.broadcasted_iota(jnp.int32, (512, 256), 0)
    q = lax.broadcasted_iota(jnp.int32, (512, 256), 1)
    U = jnp.zeros((512, 256), F32)
    for o in (0, PS):
        th, tl = split2(yr[o : o + PS, :].T)
        U = U + nn(left3(th, tl), right3(*split2(yc[o : o + PS, :])))
    at = [pl.ds(pl.multiple_of(j * 16 + o, 16), 16) for o in (0, PS)]
    cols = jnp.concatenate([yr[at[0], :], yr[at[1], :], jnp.zeros((96, 512), F32)], 0).T
    rm = r % 256
    posrow = jnp.where(rm < 32, (rm // 16) * 512 + (2 * i + r // 256) * 16 + rm % 16, 1024)
    poscol = (q // 16) * 512 + j * 16 + q % 16
    damp = damp_ref[0:1, :]
    damp2 = jnp.concatenate([damp, damp], axis=1)
    A = a_ref[...] + jnp.where(r + 512 * i == q + 256 * j, damp2, 0.0)
    cols = jnp.concatenate([cols, jnp.zeros((512, 128), F32)], 1)
    out_ref[...] = jnp.where(
        q >= 32, jnp.where(rm >= 32, A - U, 0.0), jnp.where(posrow >= poscol, cols, 0.0))


def on_device(factors):
    vm = pl.BlockSpec(memory_space=pltpu.VMEM)
    dma = pltpu.SemaphoreType.DMA
    v = pltpu.VMEM
    f = jax.ShapeDtypeStruct
    parts = pl.pallas_call(
        kernel,
        out_shape=[f((1024, 512), F32), f((1024, 256), F32), f((8, 128), F32)],
        in_specs=[vm],
        out_specs=[vm] * 3,
        scratch_shapes=[
            v((2, 16, 2, 16, 1024), F32), v((2, 16, 2, 16, 256), F32),
            v((2, 16, 2, 16, 512), F32), v((2, 16, 2, 8, 128), F32), v((16, 2, 1, 128), F32), v((16, 1, 128), F32),
            v((NB, NB), F32), v((4, NB, 3 * NB), BF16), v((PS, PS), BF16), v((PS, PS), BF16), v((PS, PS), BF16),
            v((PS, PS), BF16), v((PS, PS), F32), v((PS, RW), F32), v((PS, RW), BF16), v((PS, RW), BF16),
            v((NB, NB), F32),
            dma((16,)), dma((16,)), dma((6,)), dma((16,)), dma((16,)), dma((16,)), dma((16,)), dma((16,)), dma((16,)),
            dma((3, 16)), dma((3, 16)), dma((2, 3, 4)), dma((16,)), dma((16,)), dma((2, 16)), dma((2, 16)),
            dma((16,)), dma((16,)),
        ],
        compiler_params=pltpu.CompilerParams(
            collective_id=0, has_side_effects=True, vmem_limit_bytes=42 * 1024 * 1024),
        name="gather_eliminate",
    )(factors[0])
    out = pl.pallas_call(
        finish,
        out_shape=f((512, 256), F32),
        in_specs=[vm] * 4,
        out_specs=vm,
        compiler_params=pltpu.CompilerParams(vmem_limit_bytes=16 * 1024 * 1024),
        name="finish",
    )(factors[0], *parts)
    return out[None]


def solution(mesh):
    placed = P(None, "row", "col")
    return jax.shard_map(on_device, mesh=mesh, in_specs=(placed,), out_specs=placed, check_vma=False)
```

```python
import jax
import jax.numpy as jnp
from jax import lax
from jax.experimental import pallas as pl
from jax.experimental.pallas import tpu as pltpu
from jax.sharding import PartitionSpec as P

F32, BF16 = jnp.float32, jnp.bfloat16
MESH = pl.DeviceIdType.MESH
damping_share = 0.03162277660168379
NB = 128
MINI = 64
AHEAD = (6, 6, 7)
PS = 512
RW = PS + 256 + 512


def split3(x):
    h = x.astype(BF16)
    r = x - h.astype(F32)
    m = r.astype(BF16)
    return h, m, (r - m.astype(F32)).astype(BF16)


def split2(x):
    h = x.astype(BF16)
    return h, (x - h.astype(F32)).astype(BF16)


def tn(a, b):
    return lax.dot_general(a, b, (((0,), (0,)), ((), ())), preferred_element_type=F32)


def nn(a, b):
    return lax.dot_general(a, b, (((1,), (0,)), ((), ())), preferred_element_type=F32)


def left3(h, l):
    return jnp.concatenate([h, l, h], axis=1)


def right3(h, l):
    return jnp.concatenate([h, h, l], axis=0)


def block_inverse(M, b=MINI, ahead=AHEAD):
    n = NB
    H = b // 8
    sub = lax.broadcasted_iota(jnp.int32, (8, n), 0)
    lane = lax.broadcasted_iota(jnp.int32, (8, n), 1)

    def spread(x, s):
        return jnp.broadcast_to(x[s : s + 1, :], (8, n))

    M = [M[8 * q : 8 * q + 8, :] for q in range(n // 8)]
    for r0 in range(0, n, b):
        q0 = r0 // 8
        N = M[q0 : q0 + H]

        def column(k):
            return [
                jnp.broadcast_to(N[h][:, r0 + k : r0 + k + 1], (8, n)) if h >= k // 8 else None for h in range(H)]

        S = {k: column(k) for k in range(ahead[0])}
        have = ahead[0]
        scale = [None] * H
        d = spread(S[0][0], 0)
        for j in range(b):
            hj, sj = j // 8, j % 8
            rs = lax.rsqrt(d)
            scale[hj] = rs if sj == 0 else jnp.where(sub == sj, rs, scale[hj])
            here = lane == r0 + j
            N[hj] = jnp.where(here, jnp.where(sub == sj, 1.0, 0.0), N[hj])
            if j == b - 1:
                break
            C = S.pop(j)
            row = {k: spread(C[k // 8], k % 8) for k in S}
            rinv = rs * rs
            hn, sn = (j + 1) // 8, (j + 1) % 8
            d = spread(S[j + 1][hn], sn) - (row[j + 1] * row[j + 1]) * rinv
            u = [C[h] * rinv if h >= hj else None for h in range(H)]
            for k in S:
                S[k] = [S[k][h] - u[h] * row[k] if h >= k // 8 else None for h in range(H)]
            prow = spread(N[hj], sj)
            for h in range(hj, H):
                if h > hj:
                    N[h] = jnp.where(here, 0.0, N[h]) - u[h] * prow
                elif sj < 7:
                    N[h] = N[h] - jnp.where(sub > sj, u[h], 0.0) * prow
            while have < min(b, j + 1 + ahead[3 * j // b]):
                S[have] = column(have)
                have += 1
        N = [N[h] * scale[h] for h in range(H)]
        for h in range(H):
            M[q0 + h] = jnp.where(lane <= sub + (r0 + 8 * h), N[h], 0.0)
        if r0 + b < n:
            X = [
                jnp.where((lane > sub + (r0 + 8 * h)) & (lane < r0 + b), 0.0, N[h]) for h in range(H)]
            h_, m_, l_ = split3(jnp.concatenate(X, axis=0))
            R = tn(jnp.concatenate([h_, h_, m_, h_, l_, m_], 0), jnp.concatenate([h_, m_, h_, l_, h_, m_], 0))
            inblk = (lane >= r0) & (lane < r0 + b)
            for q in range(q0 + H, n // 8):
                M[q] = jnp.where(inblk, 0.0, M[q]) - R[8 * q : 8 * q + 8, :]
    return jnp.concatenate(M, axis=0)


def kernel(a_ref, yr, yc, damp_ref, akk, bc, br, zb, tz, tx, dn, wst, lh, ll, kh, kl, g0, g1, ph, pm,
           w_ref, zs, zr, zd, vs, vr, ts, tr, xs, xr, ks, kr, kd, hs, hr, us, ur, ds, dr):
    i = lax.axis_index("row")
    j = lax.axis_index("col")
    z = j // 2
    c = lax.rem(j, 2)
    partner = (i, 2 * z + 1 - c)

    def zpeer(d):
        return (i, 2 * lax.rem(z + d, 16) + c)

    def xpeer(d):
        return (lax.rem(i + d, 16), j)

    def copy(src, dst, ssem, rsem, dev):
        return pltpu.make_async_remote_copy(
            src_ref=src, dst_ref=dst, send_sem=ssem, recv_sem=rsem, device_id=dev, device_id_type=MESH)

    def each(lo, hi, f):
        def step(d, carry):
            f(d)
            return carry
        lax.fori_loop(lo, hi, step, 0)

    barrier = pltpu.get_barrier_semaphore()

    def greet(d):
        pl.semaphore_signal(barrier, inc=1, device_id=zpeer(d), device_id_type=MESH)
        pl.semaphore_signal(barrier, inc=1, device_id=xpeer(d), device_id_type=MESH)

    each(1, 16, greet)
    pl.semaphore_signal(barrier, inc=1, device_id=partner, device_id_type=MESH)

    lane = lax.broadcasted_iota(jnp.int32, (32, 128), 1)
    V = jnp.concatenate([a_ref[0:32, 0:128], a_ref[256:288, 0:128], jnp.zeros((64, 128), F32)], 0).T[0:32, :]
    v0 = jnp.where(lane < 16, V, pltpu.roll(V, 112, 1))
    v1 = jnp.where(lane < 16, pltpu.roll(V, 112, 1), pltpu.roll(V, 96, 1))
    part = lane[0:8, :]
    zb[0, z, c] = jnp.where(
        part < 32, v0[0:8, :],
        jnp.where(part < 64, pltpu.roll(v0[8:16, :], 32, 1),
                  jnp.where(part < 96, pltpu.roll(v0[16:24, :], 64, 1), pltpu.roll(v0[24:32, :], 96, 1))))
    zb[1, z, c] = jnp.where(part < 32, v1[16:24, :], pltpu.roll(v1[24:32, :], 32, 1))
    r = lax.broadcasted_iota(jnp.int32, (256, 256), 0)
    q = lax.broadcasted_iota(jnp.int32, (256, 256), 1)
    own = a_ref[pl.ds(pl.multiple_of(256 * c, 256), 256), :]
    t = jnp.sum(jnp.where((r == q) & (z == i), own, 0.0), axis=0, keepdims=True)
    tz[z, c] = jnp.broadcast_to(jnp.sum(t, axis=1, keepdims=True), (1, 128))

    pl.semaphore_wait(barrier, 31)

    def behind(v, d):
        return lax.rem(v + 16 - d, 16)

    def z_copy(d, s):
        return copy(zb.at[0, s, c], zb.at[0, s, c], zs.at[d], zr.at[d], zpeer(d))

    def v_copy(d, s):
        return copy(zb.at[1, s, c], zb.at[1, s, c], vs.at[d], vr.at[d], zpeer(d))

    def t_copy(d, s):
        return copy(tz.at[s, c], tz.at[s, c], ts.at[d], tr.at[d], zpeer(d))

    def x_copy(d, s):
        return copy(bc.at[:, s], bc.at[:, s], xs.at[d], xr.at[d], xpeer(d))

    def h_copy(d, s):
        return copy(tx.at[s], tx.at[s], hs.at[d], hr.at[d], xpeer(d))

    def lanes(n, x):
        return pl.ds(512, 512) if n == 1 else pl.ds((512 if n else 0) + NB * x, 512 - NB * x)

    def k_send(n, x, d):
        v = akk.at[n // 2, i, c, :, lanes(n, x)]
        return copy(v, v, ks.at[n, d], kr.at[n, i], xpeer(d))

    def k_sends(n, f):
        for x in range(1 if n == 1 else 4):
            if n == 1:
                each(1, 16, lambda d: f(k_send(n, x, d)))
            else:

                @pl.when(i // 4 == x)
                def _():
                    each(1, 16, lambda d: f(k_send(n, x, d)))

    def k_recv(n, xs=(0, 1, 2, 3)):
        for x in xs:

            def one(s, carry):
                @pl.when(s != i)
                def _():
                    v = akk.at[n // 2, s, c, :, lanes(n, x)]
                    copy(v, v, ks.at[n, 0], kr.at[n, s], partner).wait_recv()
                return carry

            lax.fori_loop(4 * x, 4 * x + 4, one, 0)

    def k_pair(n, x, h):
        v = akk.at[n // 2, pl.ds(4 * x, 4), h, :, lanes(n, x)]
        return copy(v, v, kd.at[0, n, x], kd.at[1, n, x], partner)

    def k_pairs(n, h, f):
        for x in range(4):
            f(k_pair(n, x, h))

    def begin(v):
        v.start()

    def arrived(v):
        v.wait_recv()

    def left(v):
        v.wait_send()

    def z_pair(h):
        return copy(zb.at[0, :, h], zb.at[0, :, h], zd.at[0], zd.at[1], partner)

    def v_pair(h):
        return copy(zb.at[1, :, h], zb.at[1, :, h], zd.at[4], zd.at[5], partner)

    def t_pair(h):
        return copy(tz.at[:, h], tz.at[:, h], zd.at[2], zd.at[3], partner)

    up_to = (i, 2 * lax.rem(z + 1, 16) + c)
    down_to = (i, 2 * lax.rem(z + 15, 16) + c)

    def ring(s, up, arriving=False):
        e = s + 1 if arriving else s
        k = behind(z, e) if up else lax.rem(z + e, 16)
        o = 0 if up else 8
        return [
            copy(br.at[p, k, c], br.at[p, k, c], us.at[p, s + o], ur.at[p, s + o], up_to if up else down_to)
            for p in range(2)]

    def pair(k, h):
        return copy(br.at[:, k, h], br.at[:, k, h], ds.at[k], dr.at[k], partner)

    def ring_step(s):
        for p in range(2):
            ring(s - 1, True, True)[p].wait_recv()
            ring(s, True)[p].start()
            ring(s - 1, False, True)[p].wait_recv()
            if s < 7:
                ring(s, False)[p].start()
        pair(behind(z, s), c).start()
        pair(lax.rem(z + s, 16), c).start()

    def ring_end():
        for p in range(2):
            ring(7, True, True)[p].wait_recv()
        pair(lax.rem(z + 8, 16), c).start()

    def assembled(n):
        p = zb[n].reshape(32, 1, 8, 128)
        two = pltpu.roll(p.reshape(256, 128), 96, 1).reshape(32, 1, 8, 128)
        return jnp.concatenate([p, two], axis=1).reshape(512, 128).T

    each(1, 16, lambda d: z_copy(d, z).start())
    each(1, 16, lambda d: t_copy(d, z).start())
    T = a_ref[:, 0:128].T
    br[0, z, c] = T[0:16, :]
    br[1, z, c] = T[16:32, :]
    for p in range(2):
        for h in range(2):
            bc[p, i, h] = a_ref[256 * h + 16 * p : 256 * h + 16 * p + 16, :]
    for p in range(2):
        ring(0, True)[p].start()
        ring(0, False)[p].start()
    each(1, 16, lambda d: v_copy(d, z).start())
    pair(z, c).start()
    each(1, 16, lambda d: x_copy(d, i).start())
    each(1, 16, lambda d: z_copy(d, behind(z, d)).wait_recv())
    z_pair(c).start()
    each(1, 16, lambda d: t_copy(d, behind(z, d)).wait_recv())
    t_pair(c).start()
    ring_step(1)
    z_pair(1 - c).wait_recv()
    S = assembled(0)
    akk[0, i, c, :, 0:512] = jnp.where(c == 0, S[0:16, :], S[16:32, :])
    t_pair(1 - c).wait_recv()
    tx[i] = jnp.sum(tz[...].reshape(32, 1, 128), axis=0)
    each(1, 16, lambda d: h_copy(d, i).start())
    k_sends(0, begin)
    ring_step(2)
    akk[0, i, c, :, 512:1024] = jnp.where(c == 0, S[64:80, :], S[80:96, :])
    each(1, 16, lambda d: v_copy(d, behind(z, d)).wait_recv())
    v_pair(c).start()
    v_pair(1 - c).wait_recv()
    ring_step(3)
    S = assembled(1)
    akk[1, i, c, :, 512:1024] = jnp.where(c == 0, S[0:16, :], S[16:32, :])
    each(1, 16, lambda d: h_copy(d, behind(i, d)).wait_recv())
    damp = jnp.sum(tx[...], axis=0) * (damping_share / 8192.0)
    damp_ref[...] = jnp.broadcast_to(damp, (8, 128))
    k_recv(0, (0,))
    k_pair(0, 0, c).start()
    k_recv(0, (1, 2, 3))
    for x in (1, 2, 3):
        k_pair(0, x, c).start()
    k_sends(1, begin)
    k_sends(2, begin)
    ring_step(4)
    k_pair(0, 0, 1 - c).wait_recv()

    damp2 = jnp.concatenate([damp, damp], axis=1)
    damp4 = jnp.concatenate([damp2, damp2], axis=1)
    eye = lax.broadcasted_iota(jnp.int32, (NB, NB), 0) == lax.broadcasted_iota(jnp.int32, (NB, NB), 1)
    deye = jnp.where(eye, damp, 0.0)
    ln = lax.broadcasted_iota(jnp.int32, (PS, 512), 1)
    posl = jnp.where(ln % 256 < 32, (ln % 256 // 16) * 512 + (2 * i + ln // 256) * 16 + ln % 16, -1)
    posr = lax.broadcasted_iota(jnp.int32, (PS, 512), 0)

    dn[...] = akk[0, 0:4, :, :, 0:NB].reshape(NB, NB)

    def middle():
        each(1, 16, lambda d: x_copy(d, behind(i, d)).wait_recv())
        k_pairs(1, 1 - c, arrived)
        k_pairs(2, 1 - c, arrived)
        each(0, 16, lambda k: pair(k, 1 - c).wait_recv())
        for b in range(4):
            o = b * NB
            rows = slice(o, o + NB)
            acc = jnp.concatenate([
                akk[0, 4 * b : 4 * b + 4, :, :, 512:1024].reshape(NB, 512),
                bc[0, 4 * b : 4 * b + 4].reshape(NB, 256),
                br[0, 4 * b : 4 * b + 4].reshape(NB, 512) + jnp.where(posr[rows] == posl[rows], damp4, 0.0)], axis=1)
            if b:
                acc = acc - nn(
                    jnp.concatenate([lh[rows, 0:o], ll[rows, 0:o], lh[rows, 0:o]], axis=1),
                    jnp.concatenate([ph[0:o, :], ph[0:o, :], pm[0:o, :]], axis=0))
            Y = nn(wst[b], right3(*split2(acc)))
            yr[rows, :] = Y[:, PS + 256 :]
            yc[rows, :] = Y[:, PS : PS + 256]
            ph[rows, :], pm[rows, :] = split2(Y)
            th, tl = split2(Y[:, 0:PS].T)
            kh[:, o : o + NB] = th
            kl[:, o : o + NB] = tl
        lhs = jnp.concatenate([kh[...], kl[...], kh[...]], axis=1)
        for o in range(0, RW, 256):
            R = nn(lhs, jnp.concatenate([ph[:, o : o + 256], ph[:, o : o + 256], pm[:, o : o + 256]], axis=0))
            if o < PS:
                src = akk[1, :, :, :, 512 + o : 768 + o].reshape(512, 256)
            elif o == PS:
                src = bc[1].reshape(512, 256)
            else:
                v = o - PS - 256
                src = br[1, :, :, :, v : v + 256].reshape(512, 256) + jnp.where(
                    posr[:, v : v + 256] + 512 == posl[:, v : v + 256], damp2, 0.0)
            g1[:, o : o + 256] = src - R
        dn[...] = g1[0:NB, 0:NB]

    def body(b, carry):
        w_ref[...] = block_inverse(dn[...] + deye)
        for k in range(8):

            @pl.when(b == k)
            def _():
                wl = left3(*split2(w_ref[...]))
                kk = k % 4
                lo = (kk + 1) * NB
                rows = slice(kk * NB, lo)
                if k < 4:
                    wst[k] = wl
                    if k < 3:
                        ring_step(5 + k)
                    if k == 0:
                        for x in (1, 2, 3):
                            k_pair(0, x, 1 - c).wait_recv()
                        g0[...] = akk[0, :, :, :, 0:512].reshape(512, 512)
                    if k == 2:
                        k_recv(1)
                        k_pairs(1, c, begin)
                        k_recv(2)
                        ring_end()
                        k_pairs(2, c, begin)
                    if k == 3:
                        middle()
                        return
                    g, hi = g0, PS
                else:
                    g, hi = g1, RW
                Y = nn(wl, right3(*split2(g[rows, lo:hi])))
                h, l = split2(Y)
                if k >= 4:
                    yr[PS + kk * NB : PS + lo, :] = Y[:, PS + 256 - lo :]
                    yc[PS + kk * NB : PS + lo, :] = Y[:, PS - lo : PS + 256 - lo]
                if kk < 3:
                    th, tl = split2(Y[:, 0 : PS - lo].T)
                    if k < 4:
                        lh[lo:PS, rows] = th
                        ll[lo:PS, rows] = tl
                    lhs = left3(th, tl)
                    right = right3(h, l)
                    for o in range(0, hi - lo, 256):
                        e = min(o + 256, hi - lo)
                        g[lo:PS, lo + o : lo + e] = g[lo:PS, lo + o : lo + e] - nn(lhs, right[:, o:e])
                    dn[...] = g[lo : lo + NB, lo : lo + NB]
        return carry

    lax.fori_loop(0, 8, body, 0)

    each(1, 16, lambda d: z_copy(d, z).wait_send())
    each(1, 16, lambda d: v_copy(d, z).wait_send())
    v_pair(c).wait_send()
    each(1, 16, lambda d: t_copy(d, z).wait_send())
    each(1, 16, lambda d: x_copy(d, i).wait_send())
    each(1, 16, lambda d: h_copy(d, i).wait_send())
    for n in range(3):
        k_sends(n, left)
        k_pairs(n, c, left)
    for s in range(8):
        for p in range(2):
            ring(s, True)[p].wait_send()
            if s < 7:
                ring(s, False)[p].wait_send()
    each(0, 16, lambda k: pair(k, c).wait_send())
    z_pair(c).wait_send()
    t_pair(c).wait_send()


def finish(a_ref, yr, yc, damp_ref, out_ref):
    i = lax.axis_index("row")
    j = lax.axis_index("col")
    r = lax.broadcasted_iota(jnp.int32, (512, 256), 0)
    q = lax.broadcasted_iota(jnp.int32, (512, 256), 1)
    U = jnp.zeros((512, 256), F32)
    for o in (0, PS):
        th, tl = split2(yr[o : o + PS, :].T)
        U = U + nn(left3(th, tl), right3(*split2(yc[o : o + PS, :])))
    at = [pl.ds(pl.multiple_of(j * 16 + o, 16), 16) for o in (0, PS)]
    cols = jnp.concatenate([yr[at[0], :], yr[at[1], :], jnp.zeros((96, 512), F32)], 0).T
    rm = r % 256
    posrow = jnp.where(rm < 32, (rm // 16) * 512 + (2 * i + r // 256) * 16 + rm % 16, 1024)
    poscol = (q // 16) * 512 + j * 16 + q % 16
    damp = damp_ref[0:1, :]
    damp2 = jnp.concatenate([damp, damp], axis=1)
    A = a_ref[...] + jnp.where(r + 512 * i == q + 256 * j, damp2, 0.0)
    cols = jnp.concatenate([cols, jnp.zeros((512, 128), F32)], 1)
    out_ref[...] = jnp.where(
        q >= 32, jnp.where(rm >= 32, A - U, 0.0), jnp.where(posrow >= poscol, cols, 0.0))


def on_device(factors):
    vm = pl.BlockSpec(memory_space=pltpu.VMEM)
    dma = pltpu.SemaphoreType.DMA
    v = pltpu.VMEM
    f = jax.ShapeDtypeStruct
    parts = pl.pallas_call(
        kernel,
        out_shape=[f((1024, 512), F32), f((1024, 256), F32), f((8, 128), F32)],
        in_specs=[vm],
        out_specs=[vm] * 3,
        scratch_shapes=[
            v((2, 16, 2, 16, 1024), F32), v((2, 16, 2, 16, 256), F32),
            v((2, 16, 2, 16, 512), F32), v((2, 16, 2, 8, 128), F32), v((16, 2, 1, 128), F32), v((16, 1, 128), F32),
            v((NB, NB), F32), v((4, NB, 3 * NB), BF16), v((PS, PS), BF16), v((PS, PS), BF16), v((PS, PS), BF16),
            v((PS, PS), BF16), v((PS, PS), F32), v((PS, RW), F32), v((PS, RW), BF16), v((PS, RW), BF16),
            v((NB, NB), F32),
            dma((16,)), dma((16,)), dma((6,)), dma((16,)), dma((16,)), dma((16,)), dma((16,)), dma((16,)), dma((16,)),
            dma((3, 16)), dma((3, 16)), dma((2, 3, 4)), dma((16,)), dma((16,)), dma((2, 16)), dma((2, 16)),
            dma((16,)), dma((16,)),
        ],
        compiler_params=pltpu.CompilerParams(
            collective_id=0, has_side_effects=True, vmem_limit_bytes=42 * 1024 * 1024),
        name="gather_eliminate",
    )(factors[0])
    out = pl.pallas_call(
        finish,
        out_shape=f((512, 256), F32),
        in_specs=[vm] * 4,
        out_specs=vm,
        compiler_params=pltpu.CompilerParams(vmem_limit_bytes=16 * 1024 * 1024),
        name="finish",
    )(factors[0], *parts)
    return out[None]


def solution(mesh):
    placed = P(None, "row", "col")
    return jax.shard_map(on_device, mesh=mesh, in_specs=(placed,), out_specs=placed, check_vma=False)
```
